32 devices in a mesh: south: 8 (over z, x), east: 4 (over y, core).
Axes of the slice: x: 2, y: 2, z: 4, core: 2. Of those that a mesh axis runs over, the one named last changes fastest.
Arguments:
- tracer: float32 [256, 128, 128], P('south', 'east'), may hold values from 0.2 to 1.8
- flow_j: float32 [256, 128, 128], P('south', 'east'), may hold values from -0.3 to 0.3
- flow_i: float32 [256, 128, 128], P('south', 'east'), may hold values from -0.3 to 0.3
Outputs:
- running_total: float32 [256, 128, 128], P('south', 'east')
- tracer_end: float32 [256, 128, 128], P('south', 'east')
The draws below stay inside these ranges and needn't reach their ends.
All inputs are finite; a program needn't handle non-finite values.
Results may differ from the reference program's by a relative error of at most 0.00002.
Values sent between devices are 32-bit elements; how exact they have to be, the bound alone decides.
A program may use at most 64 MiB of HBM per device.

```python
import jax
import jax.numpy as jnp
from jax import lax

GRID_J = 256
GRID_I = 128
MEMBERS = 128
STEPS = 4


def level_of(key, shape, pieces, least, top_value):
    gain, own = 1.0, jax.random.fold_in(key, 6)
    for dim, blocks in pieces:
        heights = jnp.exp(jax.random.uniform(jax.random.fold_in(own, dim), (blocks,), jnp.float32, least / len(pieces), top_value / len(pieces)))
        gain = gain * jnp.repeat(heights, shape[dim] // blocks).reshape([-1 if axis == dim else 1 for axis in range(len(shape))])
    return gain


def setup_inputs(seed: int = 0) -> dict:
    keys = jax.random.split(jax.random.key(seed), 4)
    tracer = jnp.clip(0.2 + 1.5999999 * jax.random.uniform(keys[0], (GRID_J, GRID_I, MEMBERS), jnp.float32) ** level_of(keys[0], (GRID_J, GRID_I, MEMBERS), ((0, 8), (1, 4)), -0.2, 0.2), 0.2, 1.8)
    flow_j = jnp.clip(jax.random.uniform(keys[1], (GRID_J, GRID_I, MEMBERS), jnp.float32, -0.3, 0.3) * level_of(keys[1], (GRID_J, GRID_I, MEMBERS), ((0, 8), (1, 4)), -0.4, 0.0), -0.3, 0.3)
    flow_i = jnp.clip(jax.random.uniform(keys[2], (GRID_J, GRID_I, MEMBERS), jnp.float32, -0.3, 0.3) * level_of(keys[2], (GRID_J, GRID_I, MEMBERS), ((0, 8), (1, 4)), -0.4, 0.0), -0.3, 0.3)
    return {"tracer": tracer, "flow_j": flow_j, "flow_i": flow_i}


def inner_cells(values, dims):
    for dim in dims:
        values = lax.slice_in_dim(values, 1, values.shape[dim] - 1, axis=dim)
    return values


def side_cells(values, dim, start, dims):
    others = [other for other in dims if other != dim]
    values = inner_cells(values, others)
    return lax.slice_in_dim(values, start, start + values.shape[dim] - 2, axis=dim)


def advance(padded, flow_j, flow_i):
    middle = inner_cells(padded, (0, 1))
    lower = [side_cells(padded, dim, 0, (0, 1)) for dim in (0, 1)]
    upper = [side_cells(padded, dim, 2, (0, 1)) for dim in (0, 1)]
    slopes = [above - below for above, below in zip(upper, lower)]
    smooth_rate = 0.05
    spread = lower[0] + upper[0] + lower[1] + upper[1] - 4.0 * middle
    return middle - flow_j * slopes[0] - flow_i * slopes[1] + smooth_rate * spread


def reference(tracer, flow_j, flow_i):
    for step in range(STEPS):
        tracer = advance(jnp.pad(tracer, ((1, 1), (1, 1), (0, 0)), mode="constant"), flow_j, flow_i)
    running_total = jnp.cumsum(tracer, axis=0) / GRID_J
    return running_total, tracer
```

```python
import functools

import jax
import jax.numpy as jnp
from jax import lax
from jax.experimental import pallas as pl
from jax.experimental.pallas import tpu as pltpu
from jax.sharding import PartitionSpec as P

RATE = 0.05
PAD = 2
TILE = 8
MESH = pl.DeviceIdType.MESH
LOWER, UPPER, LEFT, RIGHT = range(4)
SIDES = ((-1, 0), (1, 0), (0, -1), (0, 1))
BACK = (UPPER, LOWER, RIGHT, LEFT)


def chunk_of(rows, most):
    return max(c for c in range(1, most + 1) if rows % c == 0)


def view(ref, row, rows, col, cols):
    return ref.at[pl.ds(row + PAD, rows), pl.ds(col + TILE, cols), :]


def line(ref, row, col, cols):
    return ref[row + PAD, pl.ds(col + TILE, cols), :]


def step(middle, lower_j, upper_j, lower_i, upper_i, flow_j, flow_i):
    spread = lower_j + upper_j + lower_i + upper_i - 4.0 * middle
    return middle - flow_j * (upper_j - lower_j) - flow_i * (upper_i - lower_i) + RATE * spread


def advance(level, flows, row, rows, col, cols):
    def at(dj, di):
        return view(level, row + dj, rows, col + di, cols)[...]

    return step(at(0, 0), at(-1, 0), at(1, 0), at(0, -1), at(0, 1),
                view(flows.at[0], row, rows, col, cols)[...], view(flows.at[1], row, rows, col, cols)[...])


def kernel(souths, easts, tracer, flow_j, flow_i, before, end, level0, level1, level2, level3, flows, halo, reply, spill,
           own, totals, ready, load_sem, send_sem, late_sem, tracer_sem, flow_sem, far_sem, step_sem, total_send, total_recv):
    J, I, M = tracer.shape
    s, e = lax.axis_index("south"), lax.axis_index("east")
    levels = (level0, level1, level2, level3)
    zeros = functools.partial(jnp.zeros, dtype=jnp.float32)
    loads = [pltpu.make_async_copy(src, view(dst, 0, J, 0, I), load_sem.at[k])
             for k, (src, dst) in enumerate(((tracer, level0), (flow_j, flows.at[0]), (flow_i, flows.at[1])))]
    for load in loads:
        load.start()
    exists = (s > 0, s < souths - 1, e > 0, e < easts - 1)

    def peer(side):
        return {"south": s + SIDES[side][0], "east": e + SIDES[side][1]}

    barrier = pltpu.get_barrier_semaphore()
    near = 0
    for side in range(4):
        near = near + exists[side].astype(jnp.int32)

        @pl.when(exists[side])
        def _(side=side):
            pl.semaphore_signal(barrier, inc=1, device_id=peer(side), device_id_type=MESH)

    stages, known = [], 1
    while known < souths - 1:
        stages.append(known)
        known *= 2

    def tell(stage):
        reach = stages[stage]
        for ok, other in ((s >= reach, s - reach), (s + reach < souths, s + reach)):
            @pl.when(ok)
            def _(other=other):
                pl.semaphore_signal(ready.at[stage], inc=1, device_id={"south": other, "east": e}, device_id_type=MESH)

    def hear(stage):
        reach = stages[stage]
        pl.semaphore_wait(ready.at[stage], (s >= reach).astype(jnp.int32) + (s + reach < souths).astype(jnp.int32))

    def clear(level, row, rows, col, cols):
        view(level, row, rows, col, cols)[...] = zeros((rows, cols, M))

    def trim(k, row, rows, wide):
        for side, col in ((LEFT, -wide), (RIGHT, I)):
            pl.when(jnp.logical_not(exists[side]))(lambda col=col: clear(levels[k], row, rows, col, wide))

    with jax.named_scope("clear"):
        clear(level2, -2, 2, -2, I + 4)
        clear(level2, J, 2, -2, I + 4)
        clear(level3, -2, 1, 0, I)
        clear(level3, J + 1, 1, 0, I)
        spill[...] = zeros(spill.shape)
        for side, row in ((LOWER, -2), (UPPER, J)):
            pl.when(jnp.logical_not(exists[side]))(lambda row=row: clear(level0, row, 2, -3, I + 6))
        trim(0, 0, J, 4)
    with jax.named_scope("barw"):
        pl.semaphore_wait(barrier, near)

    def remote(side, src, dst, send, recv):
        return pltpu.make_async_remote_copy(src_ref=src, dst_ref=dst, send_sem=send, recv_sem=recv,
                                            device_id=peer(side), device_id_type=MESH)

    def block(ref, side, at_home, row, rows, col, cols):
        if side in (LOWER, UPPER):
            row = {(LOWER, True): row, (LOWER, False): J + row,
                   (UPPER, True): J - row - rows, (UPPER, False): -row - rows}[side, at_home]
        else:
            col = {(LEFT, True): col, (LEFT, False): I + col,
                   (RIGHT, True): I - col - cols, (RIGHT, False): -col - cols}[side, at_home]
        if len(ref.shape) == 4:
            return ref.at[:, pl.ds(row + PAD, rows), pl.ds(col + TILE, cols), :]
        return view(ref, row, rows, col, cols)

    def shift(side, ref, sems, *area):
        return remote(side, block(ref, side, True, *area), block(ref, side, False, *area), send_sem.at[side], sems.at[side])

    def first_tracer(side):
        if side in (LOWER, UPPER):
            return shift(side, level0, far_sem, 0, 2, 0, I)
        return shift(side, level0, tracer_sem, 0, J, 0, 4)

    def first_flows(side):
        if side in (LOWER, UPPER):
            return [shift(side, flows, far_sem, 0, 1, 0, I), shift(side, flows.at[0], far_sem, 1, 1, 0, I)]
        return [shift(side, flows, flow_sem, 0, J, 0, 3)]

    def corners(side, name):
        if name == "tracer":
            return [shift(side, level0, far_sem, 0, 2, col, 3) for col in (-3, I)]
        return [shift(side, flows, far_sem, 0, 1, col, 2) for col in (-2, I)]

    def second(side):
        row = {LOWER: 0, UPPER: J - 2}[side]
        return remote(side, view(level2, row, 2, -1, I + 2), halo.at[BACK[side], :, pl.ds(TILE - 1, I + 2), :],
                      late_sem.at[side], step_sem.at[side])

    def start(side, make):
        @pl.when(exists[side])
        def _():
            copies = make()
            for copy in copies if isinstance(copies, list) else [copies]:
                copy.start()

    def drain(sem, rows, cols):
        part = level0.at[pl.ds(0, rows), pl.ds(0, cols), :]
        pltpu.make_async_copy(part, part, sem).wait()

    def update(k, row, rows, col, cols):
        value = advance(levels[k - 1], flows, row, rows, col, cols)
        if k == 4:
            end[pl.ds(row, rows), pl.ds(col, cols), :] = value
        else:
            view(levels[k], row, rows, col, cols)[...] = value

    def sweep(k, first, last, col, cols, most):
        rows = chunk_of(last - first, most)

        def body(turn, _):
            update(k, first + turn * rows, rows, col, cols)
            return 0

        lax.fori_loop(0, (last - first) // rows, body, 0)

    with jax.named_scope("loads"):
        loads[0].wait()
        for side in (LOWER, UPPER, LEFT, RIGHT):
            start(side, lambda side=side: first_tracer(side))
        loads[1].wait()
        loads[2].wait()
    with jax.named_scope("startf"):
        for side in (LOWER, UPPER, LEFT, RIGHT):
            start(side, lambda side=side: first_flows(side))
        if stages:
            tell(0)
    with jax.named_scope("recvi"):
        for side in (LEFT, RIGHT):
            pl.when(exists[side])(lambda side=side: shift(BACK[side], level0, tracer_sem, 0, J, 0, 4).wait_recv())
        for side in (LOWER, UPPER):
            start(side, lambda side=side: corners(side, "tracer"))
    with jax.named_scope("recvif"):
        for side in (LEFT, RIGHT):
            pl.when(exists[side])(lambda side=side: shift(BACK[side], flows, flow_sem, 0, J, 0, 3).wait_recv())
        for side in (LOWER, UPPER):
            start(side, lambda side=side: corners(side, "flows"))
    for stage in range(1, len(stages)):
        hear(stage - 1)
        tell(stage)

    with jax.named_scope("middle"):
        for k in range(1, 5):
            sweep(k, k, J - k, k - 4, I + 2 * (4 - k), 7)
            if k < 4:
                trim(k, k, J - 2 * k, 4 - k)
        total = end[4]
        for row in range(5, J - 4):
            total = total + end[row]

    with jax.named_scope("recvj"):
        for side in (LOWER, UPPER):
            pl.when(exists[side])(lambda side=side: drain(far_sem.at[BACK[side]], 5, I + 4))
    with jax.named_scope("rim2"):
        for inner, outer in ((0, -1), (J - 1, J)):
            update(1, inner, 1, -3, I + 6)
            update(1, outer, 1, -2, I + 4)
            trim(1, inner, 1, 3)
            trim(1, outer, 1, 2)
        for side, outer in ((LOWER, -1), (UPPER, J)):
            pl.when(jnp.logical_not(exists[side]))(lambda outer=outer: clear(level1, outer, 1, -2, I + 4))
        for side, row in ((LOWER, 0), (UPPER, J - 2)):
            update(2, row, 2, -2, I + 4)
            trim(2, row, 2, 2)
            start(side, lambda side=side: second(side))
    with jax.named_scope("rim4"):
        for side, row, outer in ((LOWER, -1, -1), (UPPER, J - 3, J)):
            update(3, row, 4, -1, I + 2)
            trim(3, row, 4, 1)
            pl.when(jnp.logical_not(exists[side]))(lambda outer=outer: clear(level3, outer, 1, -1, I + 2))
        for side, row, outer, last, sign in ((LOWER, 0, -1, -2, -1.0), (UPPER, J - 4, J, J + 1, 1.0)):
            update(4, row, 4, 0, I)
            for r in range(4):
                total = total + end[row + r]

            @pl.when(exists[side])
            def _(side=side, outer=outer, last=last, sign=sign):
                value = advance(level3, flows, outer, 1, 0, I)[0]
                spill[side] = value + (RATE + sign * line(flows.at[0], last, 0, I)) * line(level3, outer, 0, I)

        own[...] = total + spill[LOWER] + spill[UPPER]

    def total_copy(source, other):
        return pltpu.make_async_remote_copy(
            src_ref=own, dst_ref=totals.at[source], send_sem=total_send, recv_sem=total_recv,
            device_id={"south": other, "east": e}, device_id_type=MESH)

    with jax.named_scope("give"):
        if stages:
            hear(len(stages) - 1)

        def give(turn, _):
            total_copy(s, s + turn).start()
            return 0

        lax.fori_loop(1, souths - s, give, 0)

    with jax.named_scope("recv2"):
        for side in (LOWER, UPPER):
            pl.when(exists[side])(lambda side=side: second(BACK[side]).wait_recv())
    with jax.named_scope("reply"):
        for side, sign, edge, inner, outer, close, away in (
            (LOWER, 1.0, 0, 1, -1, 1, 0), (UPPER, -1.0, J - 1, J - 2, J, 0, 1),
        ):
            @pl.when(exists[side])
            def _(side=side, sign=sign, edge=edge, inner=inner, outer=outer, close=close, away=away):
                def near_at(di, cols=I, col=0):
                    return halo[side, close, pl.ds(TILE + col + di, cols), :]

                def pair(value, at_outer):
                    none = jnp.zeros_like(value)
                    lower = (side == LOWER)
                    return (value, none) if lower else (none, value)

                reply[side, pl.ds(TILE - 1, I + 2), :] = (
                    RATE + sign * line(flows.at[0], edge, -1, I + 2)) * near_at(0, I + 2, -1)
                far = halo[side, away, pl.ds(TILE, I), :]
                outside = step(near_at(0), *pair(far, True), near_at(-1), near_at(1),
                               line(flows.at[0], outer, 0, I), line(flows.at[1], outer, 0, I))

                def here(di):
                    return reply[side, pl.ds(TILE + di, I), :]

                first = step(here(0), *pair(outside, False), here(-1), here(1),
                             line(flows.at[0], edge, 0, I), line(flows.at[1], edge, 0, I))
                then = (RATE + sign * line(flows.at[0], inner, 0, I)) * here(0)
                end[edge] = end[edge] + first
                end[inner] = end[inner] + then
                if side == LOWER:
                    spill[LOWER] = spill[LOWER] - first - then

    with jax.named_scope("sent"):
        for side in range(4):
            rows, cols = (5, I + 4) if side in (LOWER, UPPER) else (J, 10)
            pl.when(exists[side])(lambda side=side, rows=rows, cols=cols: drain(send_sem.at[side], rows, cols))
        for side in (LOWER, UPPER):
            pl.when(exists[side])(lambda side=side: second(side).wait_send())
    with jax.named_scope("take"):
        for count in range(1, souths):
            part = totals.at[pl.ds(0, count)]
            pl.when(s == count)(lambda part=part: pltpu.make_async_copy(part, part, total_recv).wait())
        before[...] = lax.fori_loop(0, s, lambda source, state: state + totals[source], spill[LOWER])
    for count in range(1, souths):
        part = totals.at[pl.ds(0, count)]
        pl.when(s == souths - 1 - count)(lambda part=part: pltpu.make_async_copy(part, part, total_send).wait())


def write_out(scale, before, end, running_out, end_out, running, sems):
    J = end.shape[0]
    parts = 2 if J % 2 == 0 else 1
    rows = J // parts
    copies = [pltpu.make_async_copy(end, end_out, sems.at[0])]
    copies[0].start()
    state = before[...]
    for part in range(parts):
        for row in range(part * rows, (part + 1) * rows):
            state = state + end[row]
            running[row] = state * scale
        area = pl.ds(part * rows, rows)
        copies.append(pltpu.make_async_copy(running.at[area], running_out.at[area], sems.at[1 + part]))
        copies[-1].start()
    for copy in copies:
        copy.wait()


def per_device(souths, easts, tracer, flow_j, flow_i):
    J, I, M = tracer.shape
    out = jax.ShapeDtypeStruct((J, I, M), jnp.float32)
    padded = (J + 2 * PAD, I + 2 * TILE, M)
    dma = pltpu.SemaphoreType.DMA
    results = pl.pallas_call(
        functools.partial(kernel, souths, easts),
        out_shape=(jax.ShapeDtypeStruct((I, M), jnp.float32), out),
        in_specs=[pl.BlockSpec(memory_space=pl.ANY)] * 3,
        out_specs=(pl.BlockSpec(memory_space=pltpu.VMEM),) * 2,
        scratch_shapes=[pltpu.VMEM(padded, jnp.float32)] * 4
        + [
            pltpu.VMEM((2,) + padded, jnp.float32),
            pltpu.VMEM((2, 2) + padded[1:], jnp.float32),
            pltpu.VMEM((2,) + padded[1:], jnp.float32),
            pltpu.VMEM((2, I, M), jnp.float32),
            pltpu.VMEM((I, M), jnp.float32),
            pltpu.VMEM((souths, I, M), jnp.float32),
            pltpu.SemaphoreType.REGULAR((max(1, (souths - 1).bit_length()),)),
            dma((3,)), dma((4,)), dma((2,)), dma((4,)), dma((4,)), dma((2,)), dma((2,)), dma, dma,
        ],
        compiler_params=pltpu.CompilerParams(collective_id=0, has_side_effects=True,
                                             vmem_limit_bytes=106 * 2 ** 19),
    )(tracer, flow_j, flow_i)
    return pl.pallas_call(
        functools.partial(write_out, 1.0 / (J * souths)),
        out_shape=(out, out),
        in_specs=[pl.BlockSpec(memory_space=pltpu.VMEM)] * 2,
        out_specs=(pl.BlockSpec(memory_space=pl.ANY),) * 2,
        scratch_shapes=[pltpu.VMEM((J, I, M), jnp.float32), pltpu.SemaphoreType.DMA((3,))],
        compiler_params=pltpu.CompilerParams(vmem_limit_bytes=2 ** 21),
    )(*results)


def solution(mesh):
    spec = P("south", "east", None)
    body = functools.partial(per_device, mesh.shape["south"], mesh.shape["east"])
    return jax.shard_map(body, mesh=mesh, in_specs=(spec,) * 3, out_specs=(spec,) * 2, check_vma=False)
```

```python
import functools

import jax
import jax.numpy as jnp
from jax import lax
from jax.experimental import pallas as pl
from jax.experimental.pallas import tpu as pltpu
from jax.sharding import PartitionSpec as P

RATE = 0.05
PAD = 2
TILE = 8
MESH = pl.DeviceIdType.MESH
LOWER, UPPER, LEFT, RIGHT = range(4)
SIDES = ((-1, 0), (1, 0), (0, -1), (0, 1))
BACK = (UPPER, LOWER, RIGHT, LEFT)


def chunk_of(rows, most):
    return max(c for c in range(1, most + 1) if rows % c == 0)


def view(ref, row, rows, col, cols):
    return ref.at[pl.ds(row + PAD, rows), pl.ds(col + TILE, cols), :]


def line(ref, row, col, cols):
    return ref[row + PAD, pl.ds(col + TILE, cols), :]


def step(middle, lower_j, upper_j, lower_i, upper_i, flow_j, flow_i):
    spread = lower_j + upper_j + lower_i + upper_i - 4.0 * middle
    return middle - flow_j * (upper_j - lower_j) - flow_i * (upper_i - lower_i) + RATE * spread


def advance(level, flows, row, rows, col, cols):
    def at(dj, di):
        return view(level, row + dj, rows, col + di, cols)[...]

    return step(at(0, 0), at(-1, 0), at(1, 0), at(0, -1), at(0, 1),
                view(flows.at[0], row, rows, col, cols)[...], view(flows.at[1], row, rows, col, cols)[...])


def kernel(souths, easts, tracer, flow_j, flow_i, before, end, level0, level1, level2, level3, flows, halo, reply, spill,
           tracer_bits, flow_bits, own, totals, ready, load_sem, send_sem, late_sem, bits_sem, side_sem, far_sem, last_sem,
           step_sem, total_send, total_recv):
    J, I, M = tracer.shape
    s, e = lax.axis_index("south"), lax.axis_index("east")
    levels = (level0, level1, level2, level3)
    zeros = functools.partial(jnp.zeros, dtype=jnp.float32)
    fields = ((tracer, level0), (flow_j, flows.at[0]), (flow_i, flows.at[1]))
    for number, part, bands in ((0, fields[:1], ((0, 2), (J - 2, 2))), (1, fields[1:], ((0, 2), (J - 2, 2))),
                                (2, fields[:1], ((2, J - 4),)), (3, fields[1:], ((2, J - 4),))):
        for src, dst in part:
            for row, rows in bands:
                pltpu.make_async_copy(src.at[pl.ds(row, rows)], view(dst, row, rows, 0, I), load_sem.at[number]).start()
    exists = (s > 0, s < souths - 1, e > 0, e < easts - 1)

    def peer(side):
        return {"south": s + SIDES[side][0], "east": e + SIDES[side][1]}

    barrier = pltpu.get_barrier_semaphore()
    near = 0
    for side in range(4):
        near = near + exists[side].astype(jnp.int32)

        @pl.when(exists[side])
        def _(side=side):
            pl.semaphore_signal(barrier, inc=1, device_id=peer(side), device_id_type=MESH)

    stages, known = [], 1
    while known < souths - 1:
        stages.append(known)
        known *= 2

    def tell(stage):
        reach = stages[stage]
        for ok, other in ((s >= reach, s - reach), (s + reach < souths, s + reach)):
            @pl.when(ok)
            def _(other=other):
                pl.semaphore_signal(ready.at[stage], inc=1, device_id={"south": other, "east": e}, device_id_type=MESH)

    def hear(stage):
        reach = stages[stage]
        pl.semaphore_wait(ready.at[stage], (s >= reach).astype(jnp.int32) + (s + reach < souths).astype(jnp.int32))

    def clear(level, row, rows, col, cols):
        view(level, row, rows, col, cols)[...] = zeros((rows, cols, M))

    def trim(k, row, rows, wide, sides=(LEFT, RIGHT)):
        for side in sides:
            col = {LEFT: -wide, RIGHT: I}[side]
            pl.when(jnp.logical_not(exists[side]))(lambda col=col: clear(levels[k], row, rows, col, wide))

    with jax.named_scope("clear"):
        clear(level2, -2, 2, -2, I + 4)
        clear(level2, J, 2, -2, I + 4)
        clear(level3, -2, 1, 0, I)
        clear(level3, J + 1, 1, 0, I)
        spill[...] = zeros(spill.shape)
        for side, row in ((LOWER, -2), (UPPER, J)):
            pl.when(jnp.logical_not(exists[side]))(lambda row=row: clear(level0, row, 2, -3, I + 6))
        trim(0, 0, J, 4)
    with jax.named_scope("barw"):
        pl.semaphore_wait(barrier, near)

    def remote(side, src, dst, send, recv):
        return pltpu.make_async_remote_copy(src_ref=src, dst_ref=dst, send_sem=send, recv_sem=recv,
                                            device_id=peer(side), device_id_type=MESH)

    def block(ref, side, at_home, row, rows, col, cols):
        if side in (LOWER, UPPER):
            row = {(LOWER, True): row, (LOWER, False): J + row,
                   (UPPER, True): J - row - rows, (UPPER, False): -row - rows}[side, at_home]
        else:
            col = {(LEFT, True): col, (LEFT, False): I + col,
                   (RIGHT, True): I - col - cols, (RIGHT, False): -col - cols}[side, at_home]
        if len(ref.shape) == 4:
            return ref.at[:, pl.ds(row + PAD, rows), pl.ds(col + TILE, cols), :]
        return view(ref, row, rows, col, cols)

    def shift(side, ref, sems, *area):
        return remote(side, block(ref, side, True, *area), block(ref, side, False, *area), send_sem.at[side], sems.at[side])

    def far_tracer(side):
        return [shift(side, level0, far_sem, 0, 2, 0, I)]

    def far_flows(side):
        return [shift(side, flows, far_sem, 0, 1, 0, I)]

    def far_last(side):
        return [shift(side, flows.at[0], last_sem, 1, 1, 0, I)]

    def side_tracer(side):
        return [shift(side, level0, side_sem, 0, J, 0, 4)]

    def side_flows(side):
        return [shift(side, flows, side_sem, 0, J, 0, 3)]

    bands = (LOWER, UPPER)

    def bits(side):
        out = []
        for band in bands:
            at = {LEFT: 0, RIGHT: I - 3}[side], {LEFT: 0, RIGHT: I - 2}[side]
            to = BACK[side] - LEFT
            out += [remote(side, view(level0, (0, J - 2)[band], 2, at[0], 3), tracer_bits.at[to, band, :, pl.ds(0, 3), :],
                           send_sem.at[side], bits_sem.at[to]),
                    remote(side, flows.at[:, pl.ds((0, J - 1)[band] + PAD, 1), pl.ds(at[1] + TILE, 2), :],
                           flow_bits.at[to, band, :, :, pl.ds(0, 2), :], send_sem.at[side], bits_sem.at[to])]
        return out

    def relay(band, side, here):
        to = side - LEFT
        row = (J, -2)[band], (J, -1)[band]
        col = {LEFT: -3, RIGHT: I}[side], {LEFT: -2, RIGHT: I}[side]
        src = ((tracer_bits.at[to, band, :, pl.ds(0, 3), :], flow_bits.at[to, band, :, :, pl.ds(0, 2), :]) if here else
               (view(level0, (0, J - 2)[band], 2, col[0], 3),
                flows.at[:, pl.ds((0, J - 1)[band] + PAD, 1), pl.ds(col[1] + TILE, 2), :]))
        dst = (view(level0, row[0], 2, col[0], 3), flows.at[:, pl.ds(row[1] + PAD, 1), pl.ds(col[1] + TILE, 2), :])
        return [remote(band, a, b, send_sem.at[band], far_sem.at[band]) for a, b in zip(src, dst)]

    def second(side):
        row = {LOWER: 0, UPPER: J - 2}[side]
        return remote(side, view(level2, row, 2, -1, I + 2), halo.at[BACK[side], :, pl.ds(TILE - 1, I + 2), :],
                      late_sem.at[side], step_sem.at[side])

    def start(side, make):
        @pl.when(exists[side])
        def _():
            for copy in make():
                copy.start()

    def drain(sem, rows, cols, ref=None):
        part = (level0 if ref is None else ref).at[..., pl.ds(0, rows), pl.ds(0, cols), :]
        pltpu.make_async_copy(part, part, sem).wait()

    def update(k, row, rows, col, cols):
        value = advance(levels[k - 1], flows, row, rows, col, cols)
        if k == 4:
            end[pl.ds(row, rows), pl.ds(col, cols), :] = value
        else:
            view(levels[k], row, rows, col, cols)[...] = value

    def sweep(k, first, last, col, cols, most):
        rows = chunk_of(last - first, most)

        def body(turn, _):
            update(k, first + turn * rows, rows, col, cols)
            return 0

        lax.fori_loop(0, (last - first) // rows, body, 0)

    def both(*makes, sides=(LOWER, UPPER)):
        for turn in range(2):
            @pl.when(lax.rem(s, 2) == turn)
            def _(turn=turn):
                for side in (sides if turn == 0 else sides[::-1]):
                    start(side, lambda side=side: [copy for make in makes for copy in make(side)])

    def share(side):
        for here in (True, False):
            @pl.when(exists[side] if here else jnp.logical_not(exists[side]))
            def _(here=here):
                if here:
                    drain(bits_sem.at[side - LEFT], 5, 4)
                for band in bands:
                    start(band, lambda band=band: relay(band, side, here))

    def strip(side):
        pl.when(exists[side])(lambda: drain(side_sem.at[BACK[side]], J, 10))
        for k in range(1, 5):
            sweep(k, k, J - k, {LEFT: k - 4, RIGHT: I - k}[side], 4, 15)
            if k < 4:
                trim(k, k, J - 2 * k, 4 - k, (side,))

    with jax.named_scope("load0"):
        drain(load_sem.at[0], 4, I)
        both(far_tracer)
    with jax.named_scope("load1"):
        drain(load_sem.at[1], 4, I, flows)
        both(far_flows)
        for side in (LEFT, RIGHT):
            start(side, lambda side=side: bits(side))
        if stages:
            tell(0)
    with jax.named_scope("load2"):
        drain(load_sem.at[2], J - 4, I)
        for side in (LEFT, RIGHT):
            start(side, lambda side=side: side_tracer(side))
    with jax.named_scope("load3"):
        drain(load_sem.at[3], J - 4, I, flows)
        for side in (LEFT, RIGHT):
            start(side, lambda side=side: side_flows(side))
    with jax.named_scope("inner"):
        for k in range(1, 5):
            sweep(k, k, J - k, k, I - 2 * k, 7)
    for turn, (early, late) in enumerate(((RIGHT, LEFT), (LEFT, RIGHT))):
        @pl.when(lax.rem(e, 2) == turn)
        def _(early=early, late=late):
            with jax.named_scope("early"):
                share(early)
                both(far_last)
                strip(early)
            with jax.named_scope("hear0"):
                for stage in range(1, len(stages) - 1):
                    hear(stage - 1)
                    tell(stage)
            with jax.named_scope("share"):
                share(late)
            with jax.named_scope("hear1"):
                for stage in range(max(1, len(stages) - 1), len(stages)):
                    hear(stage - 1)
                    tell(stage)
            with jax.named_scope("late"):
                strip(late)
    total = end[4]
    for row in range(5, J - 4):
        total = total + end[row]

    with jax.named_scope("recvj"):
        for side in (LOWER, UPPER):
            pl.when(exists[side])(lambda side=side: drain(far_sem.at[BACK[side]], 4, I + 5))
    with jax.named_scope("rim2"):
        for inner, outer in ((0, -1), (J - 1, J)):
            update(1, inner, 1, -3, I + 6)
            update(1, outer, 1, -2, I + 4)
            trim(1, inner, 1, 3)
            trim(1, outer, 1, 2)
        for side, outer in ((LOWER, -1), (UPPER, J)):
            pl.when(jnp.logical_not(exists[side]))(lambda outer=outer: clear(level1, outer, 1, -2, I + 4))
        for side, row in ((LOWER, 0), (UPPER, J - 2)):
            update(2, row, 2, -2, I + 4)
            trim(2, row, 2, 2)
            start(side, lambda side=side: [second(side)])
    with jax.named_scope("rim4"):
        for side in (LOWER, UPPER):
            pl.when(exists[side])(lambda side=side: drain(last_sem.at[BACK[side]], 1, I))
        for side, row, outer in ((LOWER, -1, -1), (UPPER, J - 3, J)):
            update(3, row, 4, -1, I + 2)
            trim(3, row, 4, 1)
            pl.when(jnp.logical_not(exists[side]))(lambda outer=outer: clear(level3, outer, 1, -1, I + 2))
        for side, row, outer, last, sign in ((LOWER, 0, -1, -2, -1.0), (UPPER, J - 4, J, J + 1, 1.0)):
            update(4, row, 4, 0, I)
            for r in range(4):
                total = total + end[row + r]

            @pl.when(exists[side])
            def _(side=side, outer=outer, last=last, sign=sign):
                value = advance(level3, flows, outer, 1, 0, I)[0]
                spill[side] = value + (RATE + sign * line(flows.at[0], last, 0, I)) * line(level3, outer, 0, I)

        own[...] = total + spill[LOWER] + spill[UPPER]

    def total_copy(source, other):
        return pltpu.make_async_remote_copy(
            src_ref=own, dst_ref=totals.at[source], send_sem=total_send, recv_sem=total_recv,
            device_id={"south": other, "east": e}, device_id_type=MESH)

    with jax.named_scope("give"):
        if stages:
            hear(len(stages) - 1)

        def give(turn, _):
            total_copy(s, s + turn).start()
            return 0

        lax.fori_loop(1, souths - s, give, 0)

    with jax.named_scope("recv2"):
        for side in (LOWER, UPPER):
            pl.when(exists[side])(lambda side=side: second(BACK[side]).wait_recv())
    with jax.named_scope("reply"):
        for side, sign, edge, inner, outer, close, away in (
            (LOWER, 1.0, 0, 1, -1, 1, 0), (UPPER, -1.0, J - 1, J - 2, J, 0, 1),
        ):
            @pl.when(exists[side])
            def _(side=side, sign=sign, edge=edge, inner=inner, outer=outer, close=close, away=away):
                def near_at(di, cols=I, col=0):
                    return halo[side, close, pl.ds(TILE + col + di, cols), :]

                def pair(value, at_outer):
                    none = jnp.zeros_like(value)
                    lower = (side == LOWER)
                    return (value, none) if lower else (none, value)

                reply[side, pl.ds(TILE - 1, I + 2), :] = (
                    RATE + sign * line(flows.at[0], edge, -1, I + 2)) * near_at(0, I + 2, -1)
                far = halo[side, away, pl.ds(TILE, I), :]
                outside = step(near_at(0), *pair(far, True), near_at(-1), near_at(1),
                               line(flows.at[0], outer, 0, I), line(flows.at[1], outer, 0, I))

                def here(di):
                    return reply[side, pl.ds(TILE + di, I), :]

                first = step(here(0), *pair(outside, False), here(-1), here(1),
                             line(flows.at[0], edge, 0, I), line(flows.at[1], edge, 0, I))
                then = (RATE + sign * line(flows.at[0], inner, 0, I)) * here(0)
                end[edge] = end[edge] + first
                end[inner] = end[inner] + then
                if side == LOWER:
                    spill[LOWER] = spill[LOWER] - first - then

    with jax.named_scope("sent"):
        for side in range(4):
            rows, cols = (5, I + 4) if side in (LOWER, UPPER) else (J + 2, 10)
            pl.when(exists[side])(lambda side=side, rows=rows, cols=cols: drain(send_sem.at[side], rows, cols))
        for side in (LOWER, UPPER):
            pl.when(exists[side])(lambda side=side: second(side).wait_send())
    with jax.named_scope("take"):
        for count in range(1, souths):
            part = totals.at[pl.ds(0, count)]
            pl.when(s == count)(lambda part=part: pltpu.make_async_copy(part, part, total_recv).wait())
        before[...] = lax.fori_loop(0, s, lambda source, state: state + totals[source], spill[LOWER])
    for count in range(1, souths):
        part = totals.at[pl.ds(0, count)]
        pl.when(s == souths - 1 - count)(lambda part=part: pltpu.make_async_copy(part, part, total_send).wait())


def write_out(scale, before, end, running_out, end_out, running, sems):
    J = end.shape[0]
    parts = 2 if J % 2 == 0 else 1
    rows = J // parts
    copies = [pltpu.make_async_copy(end, end_out, sems.at[0])]
    copies[0].start()
    state = before[...]
    for part in range(parts):
        for row in range(part * rows, (part + 1) * rows):
            state = state + end[row]
            running[row] = state * scale
        area = pl.ds(part * rows, rows)
        copies.append(pltpu.make_async_copy(running.at[area], running_out.at[area], sems.at[1 + part]))
        copies[-1].start()
    for copy in copies:
        copy.wait()


def per_device(souths, easts, tracer, flow_j, flow_i):
    J, I, M = tracer.shape
    out = jax.ShapeDtypeStruct((J, I, M), jnp.float32)
    padded = (J + 2 * PAD, I + 2 * TILE, M)
    dma = pltpu.SemaphoreType.DMA
    results = pl.pallas_call(
        functools.partial(kernel, souths, easts),
        out_shape=(jax.ShapeDtypeStruct((I, M), jnp.float32), out),
        in_specs=[pl.BlockSpec(memory_space=pl.ANY)] * 3,
        out_specs=(pl.BlockSpec(memory_space=pltpu.VMEM),) * 2,
        scratch_shapes=[pltpu.VMEM(padded, jnp.float32)] * 4
        + [
            pltpu.VMEM((2,) + padded, jnp.float32),
            pltpu.VMEM((2, 2) + padded[1:], jnp.float32),
            pltpu.VMEM((2,) + padded[1:], jnp.float32),
            pltpu.VMEM((2, I, M), jnp.float32),
            pltpu.VMEM((2, 2, 2, TILE, M), jnp.float32),
            pltpu.VMEM((2, 2, 2, 1, TILE, M), jnp.float32),
            pltpu.VMEM((I, M), jnp.float32),
            pltpu.VMEM((souths, I, M), jnp.float32),
            pltpu.SemaphoreType.REGULAR((max(1, (souths - 1).bit_length()),)),
            dma((4,)), dma((4,)), dma((2,)), dma((2,)), dma((4,)), dma((2,)), dma((2,)), dma((2,)), dma, dma,
        ],
        compiler_params=pltpu.CompilerParams(collective_id=0, has_side_effects=True,
                                             vmem_limit_bytes=106 * 2 ** 19),
    )(tracer, flow_j, flow_i)
    return pl.pallas_call(
        functools.partial(write_out, 1.0 / (J * souths)),
        out_shape=(out, out),
        in_specs=[pl.BlockSpec(memory_space=pltpu.VMEM)] * 2,
        out_specs=(pl.BlockSpec(memory_space=pl.ANY),) * 2,
        scratch_shapes=[pltpu.VMEM((J, I, M), jnp.float32), pltpu.SemaphoreType.DMA((3,))],
        compiler_params=pltpu.CompilerParams(vmem_limit_bytes=2 ** 21),
    )(*results)


def solution(mesh):
    spec = P("south", "east", None)
    body = functools.partial(per_device, mesh.shape["south"], mesh.shape["east"])
    return jax.shard_map(body, mesh=mesh, in_specs=(spec,) * 3, out_specs=(spec,) * 2, check_vma=False)
```

```python
import functools

import jax
import jax.numpy as jnp
from jax import lax
from jax.experimental import pallas as pl
from jax.experimental.pallas import tpu as pltpu
from jax.sharding import PartitionSpec as P

RATE = 0.05
PAD = 2
TILE = 8
MESH = pl.DeviceIdType.MESH
LOWER, UPPER, LEFT, RIGHT = range(4)
SIDES = ((-1, 0), (1, 0), (0, -1), (0, 1))
BACK = (UPPER, LOWER, RIGHT, LEFT)


def chunk_of(rows, most):
    return max(c for c in range(1, most + 1) if rows % c == 0)


def view(ref, row, rows, col, cols):
    return ref.at[pl.ds(row + PAD, rows), pl.ds(col + TILE, cols), :]


def line(ref, row, col, cols):
    return ref[row + PAD, pl.ds(col + TILE, cols), :]


def step(middle, lower_j, upper_j, lower_i, upper_i, flow_j, flow_i):
    spread = lower_j + upper_j + lower_i + upper_i - 4.0 * middle
    return middle - flow_j * (upper_j - lower_j) - flow_i * (upper_i - lower_i) + RATE * spread


def advance(level, flows, row, rows, col, cols):
    def at(dj, di):
        return view(level, row + dj, rows, col + di, cols)[...]

    return step(at(0, 0), at(-1, 0), at(1, 0), at(0, -1), at(0, 1),
                view(flows.at[0], row, rows, col, cols)[...], view(flows.at[1], row, rows, col, cols)[...])


def kernel(souths, easts, tracer, flow_j, flow_i, before, end, level0, level1, level2, level3, flows, halo, reply, spill,
           part, tracer_bits, flow_bits, mine, mine_bits, tally, own, totals, ready, load_sem, bits_sem, side_sem, far_sem, last_sem,
           step_sem, total_recv):
    J, I, M = tracer.shape
    s, e = lax.axis_index("south"), lax.axis_index("east")
    levels = (level0, level1, level2, level3)
    zeros = functools.partial(jnp.zeros, dtype=jnp.float32)
    exists = (s > 0, s < souths - 1, e > 0, e < easts - 1)

    def peer(side):
        return {"south": s + SIDES[side][0], "east": e + SIDES[side][1]}

    barrier = pltpu.get_barrier_semaphore()
    near = 0
    for side in range(4):
        near = near + exists[side].astype(jnp.int32)

        @pl.when(exists[side])
        def _(side=side):
            pl.semaphore_signal(barrier, inc=1, device_id=peer(side), device_id_type=MESH)

    fields = ((tracer, level0), (flow_j, flows.at[0]), (flow_i, flows.at[1]))
    for number, some, spans in ((0, fields[:1], ((0, 2), (J - 2, 2))), (1, fields[1:], ((0, 2), (J - 2, 2))),
                                (2, fields[:1], ((2, J - 4),)), (3, fields[1:], ((2, J - 4),))):
        for src, dst in some:
            for row, rows in spans:
                pltpu.make_async_copy(src.at[pl.ds(row, rows)], view(dst, row, rows, 0, I), load_sem.at[number]).start()

    stages, known = [], 1
    while known < souths - 1:
        stages.append(known)
        known *= 2

    def tell(stage):
        reach = stages[stage]
        for ok, other in ((s >= reach, s - reach), (s + reach < souths, s + reach)):
            @pl.when(ok)
            def _(other=other):
                pl.semaphore_signal(ready.at[stage], inc=1, device_id={"south": other, "east": e}, device_id_type=MESH)

    def hear(stage):
        reach = stages[stage]
        pl.semaphore_wait(ready.at[stage], (s >= reach).astype(jnp.int32) + (s + reach < souths).astype(jnp.int32))

    def clear(level, row, rows, col, cols):
        view(level, row, rows, col, cols)[...] = zeros((rows, cols, M))

    def trim(k, row, rows, wide, sides=(LEFT, RIGHT)):
        for side in sides:
            col = {LEFT: -wide, RIGHT: I}[side]
            pl.when(jnp.logical_not(exists[side]))(lambda col=col: clear(levels[k], row, rows, col, wide))

    with jax.named_scope("clear"):
        clear(level2, -2, 2, -2, I + 4)
        clear(level2, J, 2, -2, I + 4)
        clear(level3, -2, 1, 0, I)
        clear(level3, J + 1, 1, 0, I)
        spill[...] = zeros(spill.shape)
        for side, row in ((LOWER, -1), (UPPER, J)):
            pl.when(jnp.logical_not(exists[side]))(lambda row=row: clear(level0, row, 1, -3, I + 6))
        trim(0, 0, J, 4)
        for side in (LEFT, RIGHT):
            @pl.when(jnp.logical_not(exists[side]))
            def _(side=side):
                tracer_bits[side - LEFT, :, :, pl.ds((0, 2)[side - LEFT], 3), :] = zeros((2, 2, 3, M))
    with jax.named_scope("barw"):
        pl.semaphore_wait(barrier, near)

    def remote(side, src, dst, send, recv):
        return pltpu.make_async_remote_copy(src_ref=src, dst_ref=dst, send_sem=send, recv_sem=recv,
                                            device_id=peer(side), device_id_type=MESH)

    def block(ref, side, at_home, row, rows, col, cols):
        if side in (LOWER, UPPER):
            row = {(LOWER, True): row, (LOWER, False): J + row,
                   (UPPER, True): J - row - rows, (UPPER, False): -row - rows}[side, at_home]
        else:
            col = {(LEFT, True): col, (LEFT, False): I + col,
                   (RIGHT, True): I - col - cols, (RIGHT, False): -col - cols}[side, at_home]
        if len(ref.shape) == 4:
            return ref.at[:, pl.ds(row + PAD, rows), pl.ds(col + TILE, cols), :]
        return view(ref, row, rows, col, cols)

    def shift(side, ref, sems, *area):
        return remote(side, block(ref, side, True, *area), block(ref, side, False, *area), load_sem.at[side // 2], sems.at[side % (2 if sems is side_sem else 4)])

    def far_tracer(side):
        return [shift(side, level0, far_sem, 0, 1, 0, I)]

    def far_flow(side):
        return [shift(side, flows.at[0], far_sem, 0, 1, 0, I)]

    def far_part(side):
        area = pl.ds(TILE + 1, I - 2)
        return [remote(side, mine.at[side, area, :], part.at[BACK[side], area, :], load_sem.at[side // 2], far_sem.at[side])]

    def far_last(side):
        return [shift(side, flows.at[1], last_sem, 0, 1, 0, I), shift(side, flows.at[0], last_sem, 1, 1, 0, I)]

    def side_tracer(side):
        return [shift(side, level0, side_sem, 0, J, 0, 4)]

    def side_flows(side):
        return [shift(side, flows, side_sem, 0, J, 0, 3)]

    bands = (LOWER, UPPER)

    edge, nearest = (0, J - 1), (0, 1)

    def bits(side):
        out = []
        to = BACK[side] - LEFT
        for band in bands:
            three, two = {LEFT: (0, 0), RIGHT: (I - 3, I - 2)}[side]
            out += [remote(side, view(level0, (0, J - 2)[band], 2, three, 3),
                           tracer_bits.at[to, band, :, pl.ds((0, 2)[to], 3), :], load_sem.at[side // 2], bits_sem.at[to]),
                    remote(side, flows.at[:, edge[band] + PAD, pl.ds(two + TILE, 2), :],
                           flow_bits.at[to, band, :, pl.ds((0, 1)[to], 2), :], load_sem.at[side // 2], bits_sem.at[to])]
        return out

    def own_bits():
        for to, own_tracer, own_flow in ((0, (3, 0), (2, 0)), (1, (0, I - 2), (0, I - 1))):
            for band in bands:
                tracer_bits[to, band, :, pl.ds(own_tracer[0], 2), :] = view(level0, (0, J - 2)[band], 2, own_tracer[1], 2)[...]
                flow_bits[to, band, :, pl.ds(own_flow[0], 1), :] = flows[:, edge[band] + PAD, pl.ds(own_flow[1] + TILE, 1), :]

    def lone(band, middle, inside, left, right, flow_j, flow_i):
        none = jnp.zeros_like(middle)
        lower, upper = (none, inside) if band == LOWER else (inside, none)
        return step(middle, lower, upper, left, right, flow_j, flow_i)

    def relay(band, side):
        to = side - LEFT
        row = (J, -1)[band] + PAD
        three, two, one, parts = ((-3, -2, -1, -2), (I, I, I, I - 1))[to]

        def cells(src, dst, sem):
            return remote(band, src, dst, load_sem.at[0], sem.at[band])

        return [cells(tracer_bits.at[to, band, nearest[band], pl.ds((0, 2)[to], 3), :],
                      level0.at[row, pl.ds(three + TILE, 3), :], far_sem),
                cells(mine_bits.at[to, band, pl.ds(0, 3), :], part.at[BACK[band], pl.ds(parts + TILE, 3), :], far_sem),
                cells(flow_bits.at[to, band, 0, pl.ds((0, 1)[to], 2), :], flows.at[0, row, pl.ds(two + TILE, 2), :], far_sem),
                cells(flow_bits.at[to, band, 1, pl.ds(1, 1), :], flows.at[1, row, pl.ds(one + TILE, 1), :], last_sem)]

    def second(side):
        row = {LOWER: 0, UPPER: J - 2}[side]
        return remote(side, view(level2, row, 2, -1, I + 2), halo.at[BACK[side], :, pl.ds(TILE - 1, I + 2), :],
                      load_sem.at[0], step_sem.at[side])

    def start(side, make):
        @pl.when(exists[side])
        def _():
            for copy in make():
                copy.start()

    def count(sem, cells):
        area = tally.at[pl.ds(0, cells)]
        pltpu.make_async_copy(area, area, sem).wait()

    def drain(sem, rows, cols, ref=None):
        part = (level0 if ref is None else ref).at[..., pl.ds(0, rows), pl.ds(0, cols), :]
        pltpu.make_async_copy(part, part, sem).wait()

    def update(k, row, rows, col, cols):
        value = advance(levels[k - 1], flows, row, rows, col, cols)
        if k == 4:
            end[pl.ds(row, rows), pl.ds(col, cols), :] = value
        else:
            view(levels[k], row, rows, col, cols)[...] = value

    def sweep(k, first, last, col, cols, most):
        rows = chunk_of(last - first, most)

        def body(turn, _):
            update(k, first + turn * rows, rows, col, cols)
            return 0

        lax.fori_loop(0, (last - first) // rows, body, 0)

    def both(*makes, sides=(LOWER, UPPER)):
        for turn in range(2):
            @pl.when(lax.rem(s, 2) == turn)
            def _(turn=turn):
                for side in (sides if turn == 0 else sides[::-1]):
                    start(side, lambda side=side: [copy for make in makes for copy in make(side)])

    def share(side):
        to = side - LEFT
        pl.when(exists[side])(lambda: count(bits_sem.at[to], 20))
        for band in bands:
            def at(near, col):
                return tracer_bits[to, band, nearest[band] if near else 1 - nearest[band], pl.ds(col, 3), :]

            mine_bits[to, band, pl.ds(0, 3), :] = lone(band, at(True, 1), at(False, 1), at(True, 0), at(True, 2),
                                                       flow_bits[to, band, 0, pl.ds(0, 3), :],
                                                       flow_bits[to, band, 1, pl.ds(0, 3), :])
        for band in bands:
            start(band, lambda band=band: relay(band, side))

    def strip(side):
        pl.when(exists[side])(lambda: drain(side_sem.at[BACK[side] % 2], J, 10))
        for k in range(1, 5):
            sweep(k, k, J - k, {LEFT: k - 4, RIGHT: I - k}[side], 4, 15)
            if k < 4:
                trim(k, k, J - 2 * k, 4 - k, (side,))

    with jax.named_scope("load0"):
        drain(load_sem.at[0], 4, I)
        both(far_tracer)
    with jax.named_scope("load1"):
        drain(load_sem.at[1], 4, I, flows)
        for side in (LEFT, RIGHT):
            start(side, lambda side=side: bits(side))
        both(far_flow)
        for band in bands:
            row, inside = edge[band], (1, J - 2)[band]
            mine[band, pl.ds(TILE + 1, I - 2), :] = lone(
                band, *(line(level0, r, c, I - 2) for r, c in ((row, 1), (inside, 1), (row, 0), (row, 2))),
                *(line(flows.at[k], row, 1, I - 2) for k in (0, 1)))
        own_bits()
        both(far_part)
        if stages:
            tell(0)
    with jax.named_scope("load2"):
        drain(load_sem.at[2], J - 4, I)
        for side in (LEFT, RIGHT):
            start(side, lambda side=side: side_tracer(side))
    with jax.named_scope("load3"):
        drain(load_sem.at[3], J - 4, I, flows)
        for side in (LEFT, RIGHT):
            start(side, lambda side=side: side_flows(side))
    with jax.named_scope("inner"):
        for k in range(1, 5):
            sweep(k, k, J - k, k, I - 2 * k, 7)
    for turn, (early, late) in enumerate(((RIGHT, LEFT), (LEFT, RIGHT))):
        @pl.when(lax.rem(e, 2) == turn)
        def _(early=early, late=late):
            with jax.named_scope("early"):
                share(early)
                pl.when(jnp.logical_not(exists[late]))(lambda: share(late))
                strip(early)
                both(far_last)
            with jax.named_scope("hear0"):
                for stage in range(1, len(stages) - 1):
                    hear(stage - 1)
                    tell(stage)
            with jax.named_scope("share"):
                pl.when(exists[late])(lambda: share(late))
            with jax.named_scope("hear1"):
                for stage in range(max(1, len(stages) - 1), len(stages)):
                    hear(stage - 1)
                    tell(stage)
            with jax.named_scope("late"):
                strip(late)
    total = end[4]
    for row in range(5, J - 4):
        total = total + end[row]

    with jax.named_scope("recvj"):
        for side in (LOWER, UPPER):
            pl.when(exists[side])(lambda side=side: count(far_sem.at[BACK[side]], 3 * I + 14))
    with jax.named_scope("rim2"):
        for side, inner, outer, sign in ((LOWER, 0, -1, -1.0), (UPPER, J - 1, J, 1.0)):
            update(1, inner, 1, -3, I + 6)
            level1[outer + PAD, pl.ds(TILE - 2, I + 4), :] = part[side, pl.ds(TILE - 2, I + 4), :] + (
                RATE + sign * line(flows.at[0], outer, -2, I + 4)) * line(level0, inner, -2, I + 4)
            trim(1, inner, 1, 3)
            trim(1, outer, 1, 2)
        for side, outer in ((LOWER, -1), (UPPER, J)):
            pl.when(jnp.logical_not(exists[side]))(lambda outer=outer: clear(level1, outer, 1, -2, I + 4))
        for side, row in ((LOWER, 0), (UPPER, J - 2)):
            update(2, row, 2, -2, I + 4)
            trim(2, row, 2, 2)
            start(side, lambda side=side: [second(side)])
    with jax.named_scope("rim4"):
        for side, edge_row, outer, three, sign in ((LOWER, 0, -1, 0, -1.0), (UPPER, J - 1, J, J - 3, 1.0)):
            update(3, three, 3, -1, I + 2)
            trim(3, three, 3, 1)
            level3[outer + PAD, pl.ds(TILE - 1, I + 2), :] = zeros((I + 2, M))

            @pl.when(exists[side])
            def _(edge_row=edge_row, outer=outer, sign=sign):
                level3[outer + PAD, pl.ds(TILE - 1, I + 2), :] = (
                    RATE + sign * line(flows.at[0], outer, -1, I + 2)) * line(level2, edge_row, -1, I + 2)

            trim(3, outer, 1, 1)
        for row in (0, J - 4):
            update(4, row, 4, 0, I)
            for r in range(4):
                total = total + end[row + r]
    with jax.named_scope("spill"):
        for side, outer, last, sign in ((LOWER, -1, -2, -1.0), (UPPER, J, J + 1, 1.0)):
            @pl.when(exists[side])
            def _(side=side, outer=outer, last=last, sign=sign):
                count(last_sem.at[BACK[side]], 2 * I + 2)
                value = advance(level3, flows, outer, 1, 0, I)[0]
                spill[side] = value + (RATE + sign * line(flows.at[0], last, 0, I)) * line(level3, outer, 0, I)

        own[...] = total + spill[LOWER] + spill[UPPER]

    def total_copy(source, other):
        return pltpu.make_async_remote_copy(
            src_ref=own, dst_ref=totals.at[source], send_sem=load_sem.at[2], recv_sem=total_recv,
            device_id={"south": other, "east": e}, device_id_type=MESH)

    with jax.named_scope("give"):
        if stages:
            hear(len(stages) - 1)

        def give(turn, _):
            total_copy(s, s + turn).start()
            return 0

        lax.fori_loop(1, souths - s, give, 0)

    with jax.named_scope("recv2"):
        for side in (LOWER, UPPER):
            pl.when(exists[side])(lambda side=side: second(BACK[side]).wait_recv())
    with jax.named_scope("reply"):
        for side, sign, edge, inner, outer, close, away in (
            (LOWER, 1.0, 0, 1, -1, 1, 0), (UPPER, -1.0, J - 1, J - 2, J, 0, 1),
        ):
            @pl.when(exists[side])
            def _(side=side, sign=sign, edge=edge, inner=inner, outer=outer, close=close, away=away):
                def near_at(di, cols=I, col=0):
                    return halo[side, close, pl.ds(TILE + col + di, cols), :]

                def pair(value, at_outer):
                    none = jnp.zeros_like(value)
                    lower = (side == LOWER)
                    return (value, none) if lower else (none, value)

                reply[side, pl.ds(TILE - 1, I + 2), :] = (
                    RATE + sign * line(flows.at[0], edge, -1, I + 2)) * near_at(0, I + 2, -1)
                far = halo[side, away, pl.ds(TILE, I), :]
                outside = step(near_at(0), *pair(far, True), near_at(-1), near_at(1),
                               line(flows.at[0], outer, 0, I), line(flows.at[1], outer, 0, I))

                def here(di):
                    return reply[side, pl.ds(TILE + di, I), :]

                first = step(here(0), *pair(outside, False), here(-1), here(1),
                             line(flows.at[0], edge, 0, I), line(flows.at[1], edge, 0, I))
                then = (RATE + sign * line(flows.at[0], inner, 0, I)) * here(0)
                end[edge] = end[edge] + first
                end[inner] = end[inner] + then
                if side == LOWER:
                    spill[LOWER] = spill[LOWER] - first - then

    with jax.named_scope("sent"):
        for kind, sides, cells in ((0, (LOWER, UPPER), 7 * I + 20), (1, (LEFT, RIGHT), 10 * (J + 2))):
            one, two = (exists[side] for side in sides)
            pl.when(one != two)(lambda kind=kind, cells=cells: count(load_sem.at[kind], cells))
            pl.when(one & two)(lambda kind=kind, cells=cells: count(load_sem.at[kind], 2 * cells))
    with jax.named_scope("take"):
        for given in range(1, souths):
            piece = totals.at[pl.ds(0, given)]
            pl.when(s == given)(lambda piece=piece: pltpu.make_async_copy(piece, piece, total_recv).wait())
        before[...] = lax.fori_loop(0, s, lambda source, state: state + totals[source], spill[LOWER])
    for given in range(1, souths):
        piece = totals.at[pl.ds(0, given)]
        pl.when(s == souths - 1 - given)(lambda piece=piece: pltpu.make_async_copy(piece, piece, load_sem.at[2]).wait())


def write_out(scale, before, end, running_out, end_out, running, sems):
    J = end.shape[0]
    parts = 2 if J % 2 == 0 else 1
    rows = J // parts
    copies = [pltpu.make_async_copy(end, end_out, sems.at[0])]
    copies[0].start()
    state = before[...]
    for part in range(parts):
        for row in range(part * rows, (part + 1) * rows):
            state = state + end[row]
            running[row] = state * scale
        area = pl.ds(part * rows, rows)
        copies.append(pltpu.make_async_copy(running.at[area], running_out.at[area], sems.at[1 + part]))
        copies[-1].start()
    for copy in copies:
        copy.wait()


def per_device(souths, easts, tracer, flow_j, flow_i):
    J, I, M = tracer.shape
    out = jax.ShapeDtypeStruct((J, I, M), jnp.float32)
    padded = (J + 2 * PAD, I + 2 * TILE, M)
    dma = pltpu.SemaphoreType.DMA
    results = pl.pallas_call(
        functools.partial(kernel, souths, easts),
        out_shape=(jax.ShapeDtypeStruct((I, M), jnp.float32), out),
        in_specs=[pl.BlockSpec(memory_space=pl.ANY)] * 3,
        out_specs=(pl.BlockSpec(memory_space=pltpu.VMEM),) * 2,
        scratch_shapes=[pltpu.VMEM(padded, jnp.float32)] * 4
        + [
            pltpu.VMEM((2,) + padded, jnp.float32),
            pltpu.VMEM((2, 2) + padded[1:], jnp.float32),
            pltpu.VMEM((2,) + padded[1:], jnp.float32),
            pltpu.VMEM((2, I, M), jnp.float32),
            pltpu.VMEM((2,) + padded[1:], jnp.float32),
            pltpu.VMEM((2, 2, 2, TILE, M), jnp.float32),
            pltpu.VMEM((2, 2, 2, TILE, M), jnp.float32),
            pltpu.VMEM((2,) + padded[1:], jnp.float32),
            pltpu.VMEM((2, 2, TILE, M), jnp.float32),
            pltpu.VMEM((max(20 * (J + 2), 14 * I + 40), M), jnp.float32),
            pltpu.VMEM((I, M), jnp.float32),
            pltpu.VMEM((souths, I, M), jnp.float32),
            pltpu.SemaphoreType.REGULAR((max(1, (souths - 1).bit_length()),)),
            dma((4,)), dma((2,)), dma((2,)), dma((2,)), dma((2,)), dma((2,)), dma,
        ],
        compiler_params=pltpu.CompilerParams(collective_id=0, has_side_effects=True,
                                             vmem_limit_bytes=106 * 2 ** 19),
    )(tracer, flow_j, flow_i)
    return pl.pallas_call(
        functools.partial(write_out, 1.0 / (J * souths)),
        out_shape=(out, out),
        in_specs=[pl.BlockSpec(memory_space=pltpu.VMEM)] * 2,
        out_specs=(pl.BlockSpec(memory_space=pl.ANY),) * 2,
        scratch_shapes=[pltpu.VMEM((J, I, M), jnp.float32), pltpu.SemaphoreType.DMA((3,))],
        compiler_params=pltpu.CompilerParams(vmem_limit_bytes=2 ** 21),
    )(*results)


def solution(mesh):
    spec = P("south", "east", None)
    body = functools.partial(per_device, mesh.shape["south"], mesh.shape["east"])
    return jax.shard_map(body, mesh=mesh, in_specs=(spec,) * 3, out_specs=(spec,) * 2, check_vma=False)
```

```python
import functools

import jax
import jax.numpy as jnp
from jax import lax
from jax.experimental import pallas as pl
from jax.experimental.pallas import tpu as pltpu
from jax.sharding import PartitionSpec as P

RATE = 0.05
PAD = 2
TILE = 8
MESH = pl.DeviceIdType.MESH
LOWER, UPPER, LEFT, RIGHT = range(4)
SIDES = ((-1, 0), (1, 0), (0, -1), (0, 1))
BACK = (UPPER, LOWER, RIGHT, LEFT)


def chunk_of(rows, most):
    return max(c for c in range(1, most + 1) if rows % c == 0)


def view(ref, row, rows, col, cols):
    return ref.at[pl.ds(row + PAD, rows), pl.ds(col + TILE, cols), :]


def line(ref, row, col, cols):
    return ref[row + PAD, pl.ds(col + TILE, cols), :]


def step(middle, lower_j, upper_j, lower_i, upper_i, flow_j, flow_i):
    spread = lower_j + upper_j + lower_i + upper_i - 4.0 * middle
    return middle - flow_j * (upper_j - lower_j) - flow_i * (upper_i - lower_i) + RATE * spread


def advance(level, flows, row, rows, col, cols):
    def at(dj, di):
        return view(level, row + dj, rows, col + di, cols)[...]

    return step(at(0, 0), at(-1, 0), at(1, 0), at(0, -1), at(0, 1),
                view(flows.at[0], row, rows, col, cols)[...], view(flows.at[1], row, rows, col, cols)[...])


def kernel(souths, easts, tracer, flow_j, flow_i, before, end, level0, level1, level2, level3, flows, halo, reply, spill,
           part, tracer_bits, flow_bits, mine, mine_bits, tally, own, totals, ready, load_sem, bits_sem, side_sem, far_sem, last_sem,
           step_sem, total_recv):
    J, I, M = tracer.shape
    s, e = lax.axis_index("south"), lax.axis_index("east")
    levels = (level0, level1, level2, level3)
    zeros = functools.partial(jnp.zeros, dtype=jnp.float32)
    exists = (s > 0, s < souths - 1, e > 0, e < easts - 1)

    def peer(side):
        return {"south": s + SIDES[side][0], "east": e + SIDES[side][1]}

    barrier = pltpu.get_barrier_semaphore()
    near = 0
    for side in range(4):
        near = near + exists[side].astype(jnp.int32)

        @pl.when(exists[side])
        def _(side=side):
            pl.semaphore_signal(barrier, inc=1, device_id=peer(side), device_id_type=MESH)

    fields = ((tracer, level0), (flow_j, flows.at[0]), (flow_i, flows.at[1]))
    for number, some, spans in ((0, fields[:1], ((0, 2), (J - 2, 2))), (1, fields[1:], ((0, 2), (J - 2, 2))),
                                (2, fields[:1], ((2, J - 4),)), (3, fields[1:], ((2, J - 4),))):
        for src, dst in some:
            for row, rows in spans:
                pltpu.make_async_copy(src.at[pl.ds(row, rows)], view(dst, row, rows, 0, I), load_sem.at[number]).start()

    stages, known = [], 1
    while known < souths - 1:
        stages.append(known)
        known *= 2

    def tell(stage):
        reach = stages[stage]
        for ok, other in ((s >= reach, s - reach), (s + reach < souths, s + reach)):
            @pl.when(ok)
            def _(other=other):
                pl.semaphore_signal(ready.at[stage], inc=1, device_id={"south": other, "east": e}, device_id_type=MESH)

    def hear(stage):
        reach = stages[stage]
        pl.semaphore_wait(ready.at[stage], (s >= reach).astype(jnp.int32) + (s + reach < souths).astype(jnp.int32))

    def clear(level, row, rows, col, cols):
        view(level, row, rows, col, cols)[...] = zeros((rows, cols, M))

    def trim(k, row, rows, wide, sides=(LEFT, RIGHT)):
        for side in sides:
            col = {LEFT: -wide, RIGHT: I}[side]
            pl.when(jnp.logical_not(exists[side]))(lambda col=col: clear(levels[k], row, rows, col, wide))

    with jax.named_scope("clear"):
        clear(level2, -2, 2, -2, I + 4)
        clear(level2, J, 2, -2, I + 4)
        clear(level3, -2, 1, 0, I)
        clear(level3, J + 1, 1, 0, I)
        spill[...] = zeros(spill.shape)
        for side, row in ((LOWER, -1), (UPPER, J)):
            pl.when(jnp.logical_not(exists[side]))(lambda row=row: clear(level0, row, 1, -3, I + 6))
        trim(0, 0, J, 4)
        for side in (LEFT, RIGHT):
            @pl.when(jnp.logical_not(exists[side]))
            def _(side=side):
                tracer_bits[side - LEFT, :, :, pl.ds((0, 2)[side - LEFT], 3), :] = zeros((2, 2, 3, M))
    with jax.named_scope("barw"):
        pl.semaphore_wait(barrier, near)

    def remote(side, src, dst, send, recv):
        return pltpu.make_async_remote_copy(src_ref=src, dst_ref=dst, send_sem=send, recv_sem=recv,
                                            device_id=peer(side), device_id_type=MESH)

    def block(ref, side, at_home, row, rows, col, cols):
        if side in (LOWER, UPPER):
            row = {(LOWER, True): row, (LOWER, False): J + row,
                   (UPPER, True): J - row - rows, (UPPER, False): -row - rows}[side, at_home]
        else:
            col = {(LEFT, True): col, (LEFT, False): I + col,
                   (RIGHT, True): I - col - cols, (RIGHT, False): -col - cols}[side, at_home]
        if len(ref.shape) == 4:
            return ref.at[:, pl.ds(row + PAD, rows), pl.ds(col + TILE, cols), :]
        return view(ref, row, rows, col, cols)

    def shift(side, ref, sems, *area):
        return remote(side, block(ref, side, True, *area), block(ref, side, False, *area), load_sem.at[side // 2], sems.at[side % (2 if sems is side_sem else 4)])

    def far_tracer(side):
        return [shift(side, level0, far_sem, 0, 1, 0, I)]

    def far_flow(side):
        return [shift(side, flows.at[0], far_sem, 0, 1, 0, I)]

    def far_part(side):
        area = pl.ds(TILE + 1, I - 2)
        return [remote(side, mine.at[side, area, :], part.at[BACK[side], area, :], load_sem.at[side // 2], far_sem.at[side])]

    def far_last(side):
        return [shift(side, flows.at[1], last_sem, 0, 1, 0, I), shift(side, flows.at[0], last_sem, 1, 1, 0, I)]

    def side_tracer(side):
        return [shift(side, level0, side_sem, 0, J, 0, 4)]

    def side_flows(side):
        return [shift(side, flows, side_sem, 0, J, 0, 3)]

    bands = (LOWER, UPPER)

    edge, nearest = (0, J - 1), (0, 1)

    def bits(side):
        out = []
        to = BACK[side] - LEFT
        for band in bands:
            three, two = {LEFT: (0, 0), RIGHT: (I - 3, I - 2)}[side]
            out += [remote(side, view(level0, (0, J - 2)[band], 2, three, 3),
                           tracer_bits.at[to, band, :, pl.ds((0, 2)[to], 3), :], load_sem.at[side // 2], bits_sem.at[to]),
                    remote(side, flows.at[:, edge[band] + PAD, pl.ds(two + TILE, 2), :],
                           flow_bits.at[to, band, :, pl.ds((0, 1)[to], 2), :], load_sem.at[side // 2], bits_sem.at[to])]
        return out

    def own_bits():
        for to, own_tracer, own_flow in ((0, (3, 0), (2, 0)), (1, (0, I - 2), (0, I - 1))):
            for band in bands:
                tracer_bits[to, band, :, pl.ds(own_tracer[0], 2), :] = view(level0, (0, J - 2)[band], 2, own_tracer[1], 2)[...]
                flow_bits[to, band, :, pl.ds(own_flow[0], 1), :] = flows[:, edge[band] + PAD, pl.ds(own_flow[1] + TILE, 1), :]

    def lone(band, middle, inside, left, right, flow_j, flow_i):
        none = jnp.zeros_like(middle)
        lower, upper = (none, inside) if band == LOWER else (inside, none)
        return step(middle, lower, upper, left, right, flow_j, flow_i)

    def relay(band, side):
        to = side - LEFT
        row = (J, -1)[band] + PAD
        three, two, one, parts = ((-3, -2, -1, -2), (I, I, I, I - 1))[to]

        def cells(src, dst, sem):
            return remote(band, src, dst, load_sem.at[0], sem.at[band])

        return [cells(tracer_bits.at[to, band, nearest[band], pl.ds((0, 2)[to], 3), :],
                      level0.at[row, pl.ds(three + TILE, 3), :], far_sem),
                cells(mine_bits.at[to, band, pl.ds(0, 3), :], part.at[BACK[band], pl.ds(parts + TILE, 3), :], far_sem),
                cells(flow_bits.at[to, band, 0, pl.ds((0, 1)[to], 2), :], flows.at[0, row, pl.ds(two + TILE, 2), :], far_sem),
                cells(flow_bits.at[to, band, 1, pl.ds(1, 1), :], flows.at[1, row, pl.ds(one + TILE, 1), :], last_sem)]

    def second(side):
        row = {LOWER: 0, UPPER: J - 2}[side]
        return remote(side, view(level2, row, 2, -1, I + 2), halo.at[BACK[side], :, pl.ds(TILE - 1, I + 2), :],
                      load_sem.at[0], step_sem.at[side])

    def start(side, make):
        @pl.when(exists[side])
        def _():
            for copy in make():
                copy.start()

    def count(sem, cells):
        area = tally.at[pl.ds(0, cells)]
        pltpu.make_async_copy(area, area, sem).wait()

    def drain(sem, rows, cols, ref=None):
        part = (level0 if ref is None else ref).at[..., pl.ds(0, rows), pl.ds(0, cols), :]
        pltpu.make_async_copy(part, part, sem).wait()

    def update(k, row, rows, col, cols):
        value = advance(levels[k - 1], flows, row, rows, col, cols)
        if k == 4:
            end[pl.ds(row, rows), pl.ds(col, cols), :] = value
        else:
            view(levels[k], row, rows, col, cols)[...] = value

    def sweep(k, first, last, col, cols, most):
        rows = chunk_of(last - first, most)

        def body(turn, _):
            update(k, first + turn * rows, rows, col, cols)
            return 0

        lax.fori_loop(0, (last - first) // rows, body, 0)

    def both(*makes, sides=(LOWER, UPPER)):
        for turn in range(2):
            @pl.when(lax.rem(s, 2) == turn)
            def _(turn=turn):
                for side in (sides if turn == 0 else sides[::-1]):
                    start(side, lambda side=side: [copy for make in makes for copy in make(side)])

    def share(side):
        to = side - LEFT
        pl.when(exists[side])(lambda: count(bits_sem.at[to], 20))
        for band in bands:
            def at(near, col):
                return tracer_bits[to, band, nearest[band] if near else 1 - nearest[band], pl.ds(col, 3), :]

            mine_bits[to, band, pl.ds(0, 3), :] = lone(band, at(True, 1), at(False, 1), at(True, 0), at(True, 2),
                                                       flow_bits[to, band, 0, pl.ds(0, 3), :],
                                                       flow_bits[to, band, 1, pl.ds(0, 3), :])
        for band in bands:
            start(band, lambda band=band: relay(band, side))

    def strip(side):
        pl.when(exists[side])(lambda: drain(side_sem.at[BACK[side] % 2], J, 10))
        for k in range(1, 5):
            sweep(k, k, J - k, {LEFT: k - 4, RIGHT: I - k}[side], 4, 15)
            if k < 4:
                trim(k, k, J - 2 * k, 4 - k, (side,))

    with jax.named_scope("load0"):
        drain(load_sem.at[0], 4, I)
        both(far_tracer)
    with jax.named_scope("load1"):
        drain(load_sem.at[1], 4, I, flows)
        for side in (LEFT, RIGHT):
            start(side, lambda side=side: bits(side))
        both(far_flow)
        for band in bands:
            row, inside = edge[band], (1, J - 2)[band]
            mine[band, pl.ds(TILE + 1, I - 2), :] = lone(
                band, *(line(level0, r, c, I - 2) for r, c in ((row, 1), (inside, 1), (row, 0), (row, 2))),
                *(line(flows.at[k], row, 1, I - 2) for k in (0, 1)))
        own_bits()
        both(far_part)
        if stages:
            tell(0)
    with jax.named_scope("load2"):
        drain(load_sem.at[2], J - 4, I)
        for side in (LEFT, RIGHT):
            start(side, lambda side=side: side_tracer(side))
    with jax.named_scope("load3"):
        drain(load_sem.at[3], J - 4, I, flows)
        for side in (LEFT, RIGHT):
            start(side, lambda side=side: side_flows(side))
    with jax.named_scope("inner"):
        for k in range(1, 5):
            sweep(k, k, J - k, k, I - 2 * k, 7)
    for turn, (early, late) in enumerate(((RIGHT, LEFT), (LEFT, RIGHT))):
        @pl.when(lax.rem(e, 2) == turn)
        def _(early=early, late=late):
            with jax.named_scope("early"):
                share(early)
                pl.when(jnp.logical_not(exists[late]))(lambda: share(late))
                strip(early)
            with jax.named_scope("hear0"):
                for stage in range(1, len(stages) - 1):
                    hear(stage - 1)
                    tell(stage)
            with jax.named_scope("share"):
                pl.when(exists[late])(lambda: share(late))
                both(far_last)
            with jax.named_scope("hear1"):
                for stage in range(max(1, len(stages) - 1), len(stages)):
                    hear(stage - 1)
                    tell(stage)
            with jax.named_scope("late"):
                strip(late)
    total = end[4]
    for row in range(5, J - 4):
        total = total + end[row]

    with jax.named_scope("recvj"):
        for side in (LOWER, UPPER):
            pl.when(exists[side])(lambda side=side: count(far_sem.at[BACK[side]], 3 * I + 14))
    with jax.named_scope("rim2"):
        for side, inner, outer, sign in ((LOWER, 0, -1, -1.0), (UPPER, J - 1, J, 1.0)):
            update(1, inner, 1, -3, I + 6)
            level1[outer + PAD, pl.ds(TILE - 2, I + 4), :] = part[side, pl.ds(TILE - 2, I + 4), :] + (
                RATE + sign * line(flows.at[0], outer, -2, I + 4)) * line(level0, inner, -2, I + 4)
            trim(1, inner, 1, 3)
            trim(1, outer, 1, 2)
        for side, outer in ((LOWER, -1), (UPPER, J)):
            pl.when(jnp.logical_not(exists[side]))(lambda outer=outer: clear(level1, outer, 1, -2, I + 4))
        for side, row in ((LOWER, 0), (UPPER, J - 2)):
            update(2, row, 2, -2, I + 4)
            trim(2, row, 2, 2)
            start(side, lambda side=side: [second(side)])
    with jax.named_scope("rim4"):
        for side, edge_row, outer, three, sign in ((LOWER, 0, -1, 0, -1.0), (UPPER, J - 1, J, J - 3, 1.0)):
            update(3, three, 3, -1, I + 2)
            trim(3, three, 3, 1)
            level3[outer + PAD, pl.ds(TILE - 1, I + 2), :] = zeros((I + 2, M))

            @pl.when(exists[side])
            def _(edge_row=edge_row, outer=outer, sign=sign):
                level3[outer + PAD, pl.ds(TILE - 1, I + 2), :] = (
                    RATE + sign * line(flows.at[0], outer, -1, I + 2)) * line(level2, edge_row, -1, I + 2)

            trim(3, outer, 1, 1)
        for row in (0, J - 4):
            update(4, row, 4, 0, I)
            for r in range(4):
                total = total + end[row + r]
    with jax.named_scope("spill"):
        for side, outer, last, sign in ((LOWER, -1, -2, -1.0), (UPPER, J, J + 1, 1.0)):
            @pl.when(exists[side])
            def _(side=side, outer=outer, last=last, sign=sign):
                count(last_sem.at[BACK[side]], 2 * I + 2)
                value = advance(level3, flows, outer, 1, 0, I)[0]
                spill[side] = value + (RATE + sign * line(flows.at[0], last, 0, I)) * line(level3, outer, 0, I)

        own[...] = total + spill[LOWER] + spill[UPPER]

    def total_copy(source, other):
        return pltpu.make_async_remote_copy(
            src_ref=own, dst_ref=totals.at[source], send_sem=load_sem.at[2], recv_sem=total_recv,
            device_id={"south": other, "east": e}, device_id_type=MESH)

    with jax.named_scope("give"):
        if stages:
            hear(len(stages) - 1)

        def give(first, turn):
            total_copy(s, s + first + 2 * turn).start()
            return first

        for first in (1, 2):
            lax.fori_loop(0, (souths - s + 1 - first) // 2, lambda turn, _, first=first: give(first, turn), first)

    with jax.named_scope("recv2"):
        for side in (LOWER, UPPER):
            pl.when(exists[side])(lambda side=side: second(BACK[side]).wait_recv())
    with jax.named_scope("reply"):
        for side, sign, edge, inner, outer, close, away in (
            (LOWER, 1.0, 0, 1, -1, 1, 0), (UPPER, -1.0, J - 1, J - 2, J, 0, 1),
        ):
            @pl.when(exists[side])
            def _(side=side, sign=sign, edge=edge, inner=inner, outer=outer, close=close, away=away):
                def near_at(di, cols=I, col=0):
                    return halo[side, close, pl.ds(TILE + col + di, cols), :]

                def pair(value, at_outer):
                    none = jnp.zeros_like(value)
                    lower = (side == LOWER)
                    return (value, none) if lower else (none, value)

                reply[side, pl.ds(TILE - 1, I + 2), :] = (
                    RATE + sign * line(flows.at[0], edge, -1, I + 2)) * near_at(0, I + 2, -1)
                far = halo[side, away, pl.ds(TILE, I), :]
                outside = step(near_at(0), *pair(far, True), near_at(-1), near_at(1),
                               line(flows.at[0], outer, 0, I), line(flows.at[1], outer, 0, I))

                def here(di):
                    return reply[side, pl.ds(TILE + di, I), :]

                first = step(here(0), *pair(outside, False), here(-1), here(1),
                             line(flows.at[0], edge, 0, I), line(flows.at[1], edge, 0, I))
                then = (RATE + sign * line(flows.at[0], inner, 0, I)) * here(0)
                end[edge] = end[edge] + first
                end[inner] = end[inner] + then
                if side == LOWER:
                    spill[LOWER] = spill[LOWER] - first - then

    with jax.named_scope("sent"):
        for kind, sides, cells in ((0, (LOWER, UPPER), 7 * I + 20), (1, (LEFT, RIGHT), 10 * (J + 2))):
            one, two = (exists[side] for side in sides)
            pl.when(one != two)(lambda kind=kind, cells=cells: count(load_sem.at[kind], cells))
            pl.when(one & two)(lambda kind=kind, cells=cells: count(load_sem.at[kind], 2 * cells))
    with jax.named_scope("take"):
        for given in range(1, souths):
            piece = totals.at[pl.ds(0, given)]
            pl.when(s == given)(lambda piece=piece: pltpu.make_async_copy(piece, piece, total_recv).wait())
        before[...] = lax.fori_loop(0, s, lambda source, state: state + totals[source], spill[LOWER])
    for given in range(1, souths):
        piece = totals.at[pl.ds(0, given)]
        pl.when(s == souths - 1 - given)(lambda piece=piece: pltpu.make_async_copy(piece, piece, load_sem.at[2]).wait())


def write_out(scale, before, end, running_out, end_out, running, sems):
    J = end.shape[0]
    parts = 2 if J % 2 == 0 else 1
    rows = J // parts
    copies = [pltpu.make_async_copy(end, end_out, sems.at[0])]
    copies[0].start()
    state = before[...]
    for part in range(parts):
        for row in range(part * rows, (part + 1) * rows):
            state = state + end[row]
            running[row] = state * scale
        area = pl.ds(part * rows, rows)
        copies.append(pltpu.make_async_copy(running.at[area], running_out.at[area], sems.at[1 + part]))
        copies[-1].start()
    for copy in copies:
        copy.wait()


def per_device(souths, easts, tracer, flow_j, flow_i):
    J, I, M = tracer.shape
    out = jax.ShapeDtypeStruct((J, I, M), jnp.float32)
    padded = (J + 2 * PAD, I + 2 * TILE, M)
    dma = pltpu.SemaphoreType.DMA
    results = pl.pallas_call(
        functools.partial(kernel, souths, easts),
        out_shape=(jax.ShapeDtypeStruct((I, M), jnp.float32), out),
        in_specs=[pl.BlockSpec(memory_space=pl.ANY)] * 3,
        out_specs=(pl.BlockSpec(memory_space=pltpu.VMEM),) * 2,
        scratch_shapes=[pltpu.VMEM(padded, jnp.float32)] * 4
        + [
            pltpu.VMEM((2,) + padded, jnp.float32),
            pltpu.VMEM((2, 2) + padded[1:], jnp.float32),
            pltpu.VMEM((2,) + padded[1:], jnp.float32),
            pltpu.VMEM((2, I, M), jnp.float32),
            pltpu.VMEM((2,) + padded[1:], jnp.float32),
            pltpu.VMEM((2, 2, 2, TILE, M), jnp.float32),
            pltpu.VMEM((2, 2, 2, TILE, M), jnp.float32),
            pltpu.VMEM((2,) + padded[1:], jnp.float32),
            pltpu.VMEM((2, 2, TILE, M), jnp.float32),
            pltpu.VMEM((max(20 * (J + 2), 14 * I + 40), M), jnp.float32),
            pltpu.VMEM((I, M), jnp.float32),
            pltpu.VMEM((souths, I, M), jnp.float32),
            pltpu.SemaphoreType.REGULAR((max(1, (souths - 1).bit_length()),)),
            dma((4,)), dma((2,)), dma((2,)), dma((2,)), dma((2,)), dma((2,)), dma,
        ],
        compiler_params=pltpu.CompilerParams(collective_id=0, has_side_effects=True,
                                             vmem_limit_bytes=106 * 2 ** 19),
    )(tracer, flow_j, flow_i)
    return pl.pallas_call(
        functools.partial(write_out, 1.0 / (J * souths)),
        out_shape=(out, out),
        in_specs=[pl.BlockSpec(memory_space=pltpu.VMEM)] * 2,
        out_specs=(pl.BlockSpec(memory_space=pl.ANY),) * 2,
        scratch_shapes=[pltpu.VMEM((J, I, M), jnp.float32), pltpu.SemaphoreType.DMA((3,))],
        compiler_params=pltpu.CompilerParams(vmem_limit_bytes=2 ** 21),
    )(*results)


def solution(mesh):
    spec = P("south", "east", None)
    body = functools.partial(per_device, mesh.shape["south"], mesh.shape["east"])
    return jax.shard_map(body, mesh=mesh, in_specs=(spec,) * 3, out_specs=(spec,) * 2, check_vma=False)
```

```python
import functools

import jax
import jax.numpy as jnp
from jax import lax
from jax.experimental import pallas as pl
from jax.experimental.pallas import tpu as pltpu
from jax.sharding import PartitionSpec as P

RATE = 0.05
PAD = 2
TILE = 8
MESH = pl.DeviceIdType.MESH
LOWER, UPPER, LEFT, RIGHT = range(4)
SIDES = ((-1, 0), (1, 0), (0, -1), (0, 1))
BACK = (UPPER, LOWER, RIGHT, LEFT)


def chunk_of(rows, most):
    return max(c for c in range(1, most + 1) if rows % c == 0)


def view(ref, row, rows, col, cols):
    return ref.at[pl.ds(row + PAD, rows), pl.ds(col + TILE, cols), :]


def line(ref, row, col, cols):
    return ref[row + PAD, pl.ds(col + TILE, cols), :]


def step(middle, lower_j, upper_j, lower_i, upper_i, flow_j, flow_i):
    spread = lower_j + upper_j + lower_i + upper_i - 4.0 * middle
    return middle - flow_j * (upper_j - lower_j) - flow_i * (upper_i - lower_i) + RATE * spread


def advance(level, flows, row, rows, col, cols):
    def at(dj, di):
        return view(level, row + dj, rows, col + di, cols)[...]

    return step(at(0, 0), at(-1, 0), at(1, 0), at(0, -1), at(0, 1),
                view(flows.at[0], row, rows, col, cols)[...], view(flows.at[1], row, rows, col, cols)[...])


def kernel(souths, easts, tracer, flow_j, flow_i, before, end, level0, level1, level2, level3, flows, halo, reply, spill,
           part, tracer_bits, flow_bits, mine, mine_bits, tally, own, totals, ready, load_sem, bits_sem, side_sem, far_sem, last_sem,
           step_sem, total_recv, diag_sem, greeted):
    J, I, M = tracer.shape
    s, e = lax.axis_index("south"), lax.axis_index("east")
    levels = (level0, level1, level2, level3)
    zeros = functools.partial(jnp.zeros, dtype=jnp.float32)
    exists = (s > 0, s < souths - 1, e > 0, e < easts - 1)

    def peer(side):
        return {"south": s + SIDES[side][0], "east": e + SIDES[side][1]}

    barrier = pltpu.get_barrier_semaphore()
    near = 0
    for side in range(4):
        near = near + exists[side].astype(jnp.int32)

        @pl.when(exists[side])
        def _(side=side):
            pl.semaphore_signal(barrier, inc=1, device_id=peer(side), device_id_type=MESH)

    fields = ((tracer, level0), (flow_j, flows.at[0]), (flow_i, flows.at[1]))
    for number, some, spans in ((0, fields[:1], ((0, 2), (J - 2, 2))), (1, fields[1:], ((0, 2), (J - 2, 2))),
                                (2, fields[:1], ((2, J - 4),)), (3, fields[1:], ((2, J - 4),))):
        for src, dst in some:
            for row, rows in spans:
                pltpu.make_async_copy(src.at[pl.ds(row, rows)], view(dst, row, rows, 0, I), load_sem.at[number]).start()

    stages, known = [], 1
    while known < souths - 1:
        stages.append(known)
        known *= 2

    def tell(stage):
        reach = stages[stage]
        for ok, other in ((s >= reach, s - reach), (s + reach < souths, s + reach)):
            @pl.when(ok)
            def _(other=other):
                pl.semaphore_signal(ready.at[stage], inc=1, device_id={"south": other, "east": e}, device_id_type=MESH)

    def hear(stage):
        reach = stages[stage]
        pl.semaphore_wait(ready.at[stage], (s >= reach).astype(jnp.int32) + (s + reach < souths).astype(jnp.int32))

    def clear(level, row, rows, col, cols):
        view(level, row, rows, col, cols)[...] = zeros((rows, cols, M))

    def trim(k, row, rows, wide, sides=(LEFT, RIGHT)):
        for side in sides:
            col = {LEFT: -wide, RIGHT: I}[side]
            pl.when(jnp.logical_not(exists[side]))(lambda col=col: clear(levels[k], row, rows, col, wide))

    with jax.named_scope("clear"):
        clear(level2, -2, 2, -2, I + 4)
        clear(level2, J, 2, -2, I + 4)
        clear(level3, -2, 1, 0, I)
        clear(level3, J + 1, 1, 0, I)
        spill[...] = zeros(spill.shape)
        for side, row in ((LOWER, -1), (UPPER, J)):
            pl.when(jnp.logical_not(exists[side]))(lambda row=row: clear(level0, row, 1, -3, I + 6))
        trim(0, 0, J, 4)
        for side in (LEFT, RIGHT):
            @pl.when(jnp.logical_not(exists[side]))
            def _(side=side):
                tracer_bits[side - LEFT, :, :, pl.ds((0, 2)[side - LEFT], 3), :] = zeros((2, 2, 3, M))
    with jax.named_scope("barw"):
        pl.semaphore_wait(barrier, near)
        for turn, late in enumerate((LEFT, RIGHT)):
            @pl.when((lax.rem(e, 2) == turn) & exists[late])
            def _(late=late):
                pl.semaphore_signal(greeted, inc=1, device_id=peer(late), device_id_type=MESH)
    later = ((lax.rem(e, 2) == 0) & exists[LEFT]) | ((lax.rem(e, 2) == 1) & exists[RIGHT])

    def remote(side, src, dst, send, recv):
        return pltpu.make_async_remote_copy(src_ref=src, dst_ref=dst, send_sem=send, recv_sem=recv,
                                            device_id=peer(side), device_id_type=MESH)

    def block(ref, side, at_home, row, rows, col, cols):
        if side in (LOWER, UPPER):
            row = {(LOWER, True): row, (LOWER, False): J + row,
                   (UPPER, True): J - row - rows, (UPPER, False): -row - rows}[side, at_home]
        else:
            col = {(LEFT, True): col, (LEFT, False): I + col,
                   (RIGHT, True): I - col - cols, (RIGHT, False): -col - cols}[side, at_home]
        if len(ref.shape) == 4:
            return ref.at[:, pl.ds(row + PAD, rows), pl.ds(col + TILE, cols), :]
        return view(ref, row, rows, col, cols)

    def shift(side, ref, sems, *area):
        return remote(side, block(ref, side, True, *area), block(ref, side, False, *area), load_sem.at[side // 2], sems.at[side % (2 if sems is side_sem else 4)])

    def far_tracer(side):
        return [shift(side, level0, far_sem, 0, 1, 0, I)]

    def far_flow(side):
        return [shift(side, flows.at[0], far_sem, 0, 1, 0, I)]

    def far_part(side):
        area = pl.ds(TILE + 1, I - 2)
        return [remote(side, mine.at[side, area, :], part.at[BACK[side], area, :], load_sem.at[side // 2], far_sem.at[side])]

    def far_last(side):
        return [shift(side, flows.at[1], last_sem, 0, 1, 0, I), shift(side, flows.at[0], last_sem, 1, 1, 0, I)]

    def side_tracer(side):
        return [shift(side, level0, side_sem, 0, J, 0, 4)]

    def side_flows(side):
        return [shift(side, flows, side_sem, 0, J, 0, 3)]

    bands = (LOWER, UPPER)

    edge, nearest = (0, J - 1), (0, 1)

    def bits(side):
        out = []
        to = BACK[side] - LEFT
        for band in bands:
            three, two = {LEFT: (0, 0), RIGHT: (I - 3, I - 2)}[side]
            out += [remote(side, view(level0, (0, J - 2)[band], 2, three, 3),
                           tracer_bits.at[to, band, :, pl.ds((0, 2)[to], 3), :], load_sem.at[side // 2], bits_sem.at[to]),
                    remote(side, flows.at[:, edge[band] + PAD, pl.ds(two + TILE, 2), :],
                           flow_bits.at[to, band, :, pl.ds((0, 1)[to], 2), :], load_sem.at[side // 2], bits_sem.at[to])]
        return out

    def own_bits():
        for to, own_tracer, own_flow in ((0, (3, 0), (2, 0)), (1, (0, I - 2), (0, I - 1))):
            for band in bands:
                tracer_bits[to, band, :, pl.ds(own_tracer[0], 2), :] = view(level0, (0, J - 2)[band], 2, own_tracer[1], 2)[...]
                flow_bits[to, band, :, pl.ds(own_flow[0], 1), :] = flows[:, edge[band] + PAD, pl.ds(own_flow[1] + TILE, 1), :]

    def lone(band, middle, inside, left, right, flow_j, flow_i):
        none = jnp.zeros_like(middle)
        lower, upper = (none, inside) if band == LOWER else (inside, none)
        return step(middle, lower, upper, left, right, flow_j, flow_i)

    def relay(band, side):
        to = side - LEFT
        row = (J, -1)[band] + PAD
        three, two, parts = ((-3, -2, -2), (I, I, I - 1))[to]

        def cells(src, dst, sem):
            return remote(band, src, dst, load_sem.at[0], sem.at[band])

        return [cells(tracer_bits.at[to, band, nearest[band], pl.ds((0, 2)[to], 3), :],
                      level0.at[row, pl.ds(three + TILE, 3), :], far_sem),
                cells(mine_bits.at[to, band, pl.ds(0, 3), :], part.at[BACK[band], pl.ds(parts + TILE, 3), :], far_sem),
                cells(flow_bits.at[to, band, 0, pl.ds((0, 1)[to], 2), :], flows.at[0, row, pl.ds(two + TILE, 2), :], far_sem)]

    def cell(band, side):
        area = pl.ds({LEFT: 0, RIGHT: I - 1}[side] + TILE, 1)
        row = (J + 1, -2)[band] + PAD
        return [remote(band, level0.at[(1, J - 2)[band] + PAD, area, :], level0.at[row, area, :], load_sem.at[0], far_sem.at[band]),
                remote(band, flows.at[1, edge[band] + PAD, area, :], flows.at[1, row, area, :], load_sem.at[0], far_sem.at[band])]

    def diagonal(band, side):
        row = (J, -1)[band] + PAD, (J + 1, -2)[band] + PAD
        home, away = {LEFT: ((0, 0), (I, I)), RIGHT: ((I - 3, I - 2), (-3, -2))}[side]

        def cells(src, dst):
            return pltpu.make_async_remote_copy(
                src_ref=src, dst_ref=dst, send_sem=load_sem.at[3], recv_sem=diag_sem.at[band],
                device_id={"south": s + SIDES[band][0], "east": e + SIDES[side][1]}, device_id_type=MESH)

        return [cells(view(level0, (0, J - 2)[band], 2, home[0], 3), view(level0, (J, -2)[band], 2, away[0], 3))] + [
            cells(flows.at[k, edge[band] + PAD, pl.ds(home[1] + TILE, 2), :], flows.at[k, row[k], pl.ds(away[1] + TILE, 2), :])
            for k in (0, 1)]

    def second(side):
        row = {LOWER: 0, UPPER: J - 2}[side]
        return remote(side, view(level2, row, 2, -1, I + 2), halo.at[BACK[side], :, pl.ds(TILE - 1, I + 2), :],
                      load_sem.at[0], step_sem.at[side])

    def start(side, make):
        @pl.when(exists[side])
        def _():
            for copy in make():
                copy.start()

    def count(sem, cells):
        area = tally.at[pl.ds(0, cells)]
        pltpu.make_async_copy(area, area, sem).wait()

    def drain(sem, rows, cols, ref=None):
        part = (level0 if ref is None else ref).at[..., pl.ds(0, rows), pl.ds(0, cols), :]
        pltpu.make_async_copy(part, part, sem).wait()

    def update(k, row, rows, col, cols):
        value = advance(levels[k - 1], flows, row, rows, col, cols)
        if k == 4:
            end[pl.ds(row, rows), pl.ds(col, cols), :] = value
        else:
            view(levels[k], row, rows, col, cols)[...] = value

    def sweep(k, first, last, col, cols, most):
        rows = chunk_of(last - first, most)

        def body(turn, _):
            update(k, first + turn * rows, rows, col, cols)
            return 0

        lax.fori_loop(0, (last - first) // rows, body, 0)

    def both(*makes, sides=(LOWER, UPPER)):
        for turn in range(2):
            @pl.when(lax.rem(s, 2) == turn)
            def _(turn=turn):
                for side in (sides if turn == 0 else sides[::-1]):
                    start(side, lambda side=side: [copy for make in makes for copy in make(side)])

    def share(side):
        to = side - LEFT
        pl.when(exists[side])(lambda: count(bits_sem.at[to], 20))
        for band in bands:
            def at(near, col):
                return tracer_bits[to, band, nearest[band] if near else 1 - nearest[band], pl.ds(col, 3), :]

            mine_bits[to, band, pl.ds(0, 3), :] = lone(band, at(True, 1), at(False, 1), at(True, 0), at(True, 2),
                                                       flow_bits[to, band, 0, pl.ds(0, 3), :],
                                                       flow_bits[to, band, 1, pl.ds(0, 3), :])
        for band in bands:
            start(band, lambda band=band: relay(band, side))

    def strip(side):
        pl.when(exists[side])(lambda: drain(side_sem.at[BACK[side] % 2], J, 10))
        for k in range(1, 5):
            sweep(k, k, J - k, {LEFT: k - 4, RIGHT: I - k}[side], 4, 15)
            if k < 4:
                trim(k, k, J - 2 * k, 4 - k, (side,))

    with jax.named_scope("load0"):
        drain(load_sem.at[0], 4, I)
        both(far_tracer)
    with jax.named_scope("load1"):
        drain(load_sem.at[1], 4, I, flows)
        for turn, (early, late) in enumerate(((RIGHT, LEFT), (LEFT, RIGHT))):
            @pl.when(lax.rem(e, 2) == turn)
            def _(early=early, late=late):
                start(early, lambda: bits(early))

                @pl.when(exists[late])
                def _():
                    for band in bands:
                        start(band, lambda band=band: cell(band, late))
        both(far_flow)
        for band in bands:
            row, inside = edge[band], (1, J - 2)[band]
            mine[band, pl.ds(TILE + 1, I - 2), :] = lone(
                band, *(line(level0, r, c, I - 2) for r, c in ((row, 1), (inside, 1), (row, 0), (row, 2))),
                *(line(flows.at[k], row, 1, I - 2) for k in (0, 1)))
        own_bits()
        both(far_part)
        if stages:
            tell(0)
    with jax.named_scope("load2"):
        drain(load_sem.at[2], J - 4, I)
        for side in (LEFT, RIGHT):
            start(side, lambda side=side: side_tracer(side))
    with jax.named_scope("load3"):
        drain(load_sem.at[3], J - 4, I, flows)
        for side in (LEFT, RIGHT):
            start(side, lambda side=side: side_flows(side))
    with jax.named_scope("inner"):
        for k in range(1, 5):
            sweep(k, k, J - k, k, I - 2 * k, 7)
    def greet():
        for stage in range(1, len(stages) - 1):
            hear(stage - 1)
            tell(stage)

    for turn, (early, late) in enumerate(((RIGHT, LEFT), (LEFT, RIGHT))):
        @pl.when(lax.rem(e, 2) == turn)
        def _(early=early, late=late):
            with jax.named_scope("diag"):
                @pl.when(exists[late])
                def _():
                    pl.semaphore_wait(greeted, 1)
                    for band in bands:
                        start(band, lambda band=band: diagonal(band, late))
            with jax.named_scope("hearx"):
                pl.when(2 * e >= easts)(greet)
            with jax.named_scope("early"):
                share(early)
                pl.when(jnp.logical_not(exists[late]))(lambda: share(late))
                strip(early)
                both(far_last)
            with jax.named_scope("hear0"):
                pl.when(2 * e < easts)(greet)
            with jax.named_scope("hear1"):
                for stage in range(max(1, len(stages) - 1), len(stages)):
                    hear(stage - 1)
                    tell(stage)
            with jax.named_scope("late"):
                strip(late)
    total = end[4]
    for row in range(5, J - 4):
        total = total + end[row]

    def rim(side):
        edge_row, outer, two, three, four, sign = ((0, -1, 0, 0, 0, -1.0), (J - 1, J, J - 2, J - 3, J - 4, 1.0))[side]
        pl.when(exists[side] & jnp.logical_not(later))(lambda: count(far_sem.at[BACK[side]], 3 * I + 14))

        @pl.when(exists[side] & later)
        def _():
            count(far_sem.at[BACK[side]], 3 * I + 8)
            count(diag_sem.at[BACK[side]], 10)
        beyond = outer + outer - edge_row
        for turn, col in enumerate((-2, I - 1)):
            @pl.when((lax.rem(e, 2) == turn) & exists[side] & later)
            def _(col=col):
                part[side, pl.ds(TILE + col, 3), :] = lone(
                    BACK[side], *(line(level0, r, c, 3) for r, c in
                                  ((outer, col), (beyond, col), (outer, col - 1), (outer, col + 1))),
                    line(flows.at[0], outer, col, 3), line(flows.at[1], beyond, col, 3))
        update(1, edge_row, 1, -3, I + 6)
        trim(1, edge_row, 1, 3)
        level1[outer + PAD, pl.ds(TILE - 2, I + 4), :] = part[side, pl.ds(TILE - 2, I + 4), :] + (
            RATE + sign * line(flows.at[0], outer, -2, I + 4)) * line(level0, edge_row, -2, I + 4)
        trim(1, outer, 1, 2)
        pl.when(jnp.logical_not(exists[side]))(lambda: clear(level1, outer, 1, -2, I + 4))
        update(2, two, 2, -2, I + 4)
        trim(2, two, 2, 2)
        start(side, lambda: [second(side)])
        update(3, three, 3, -1, I + 2)
        trim(3, three, 3, 1)
        level3[outer + PAD, pl.ds(TILE - 1, I + 2), :] = zeros((I + 2, M))

        @pl.when(exists[side])
        def _():
            level3[outer + PAD, pl.ds(TILE - 1, I + 2), :] = (
                RATE + sign * line(flows.at[0], outer, -1, I + 2)) * line(level2, edge_row, -1, I + 2)

        trim(3, outer, 1, 1)
        update(4, four, 4, 0, I)

    for turn, sides in enumerate(((LOWER, UPPER), (UPPER, LOWER))):
        @pl.when(lax.rem(s, 2) == turn)
        def _(sides=sides):
            for number, side in enumerate(sides):
                with jax.named_scope(f"rim{number}"):
                    rim(side)
    for row in (*range(4), *range(J - 4, J)):
        total = total + end[row]
    with jax.named_scope("spill"):
        for side, outer, last, sign in ((LOWER, -1, -2, -1.0), (UPPER, J, J + 1, 1.0)):
            @pl.when(exists[side])
            def _(side=side, outer=outer, last=last, sign=sign):
                count(last_sem.at[BACK[side]], 2 * I)
                value = advance(level3, flows, outer, 1, 0, I)[0]
                spill[side] = value + (RATE + sign * line(flows.at[0], last, 0, I)) * line(level3, outer, 0, I)

        own[...] = total + spill[LOWER] + spill[UPPER]

    def total_copy(source, other):
        return pltpu.make_async_remote_copy(
            src_ref=own, dst_ref=totals.at[source], send_sem=load_sem.at[2], recv_sem=total_recv,
            device_id={"south": other, "east": e}, device_id_type=MESH)

    with jax.named_scope("give"):
        def give(first, lower, upper):
            def one(turn, _):
                total_copy(s, s + first + 2 * turn).start()
                return 0

            lax.fori_loop(lower, upper, one, 0)

        reach = stages[-1] if stages else souths
        for first in (1, 2):
            most = (souths - s + 1 - first) // 2
            give(first, 0, jnp.minimum(most, (reach + 2 - first) // 2))
        if stages:
            hear(len(stages) - 1)
            for first in (1, 2):
                most, done = (souths - s + 1 - first) // 2, (reach + 2 - first) // 2
                give(first, jnp.minimum(most, done), most)

    with jax.named_scope("recv2"):
        for side in (LOWER, UPPER):
            pl.when(exists[side])(lambda side=side: second(BACK[side]).wait_recv())
    with jax.named_scope("reply"):
        for side, sign, edge, inner, outer, close, away in (
            (LOWER, 1.0, 0, 1, -1, 1, 0), (UPPER, -1.0, J - 1, J - 2, J, 0, 1),
        ):
            @pl.when(exists[side])
            def _(side=side, sign=sign, edge=edge, inner=inner, outer=outer, close=close, away=away):
                def near_at(di, cols=I, col=0):
                    return halo[side, close, pl.ds(TILE + col + di, cols), :]

                def pair(value, at_outer):
                    none = jnp.zeros_like(value)
                    lower = (side == LOWER)
                    return (value, none) if lower else (none, value)

                reply[side, pl.ds(TILE - 1, I + 2), :] = (
                    RATE + sign * line(flows.at[0], edge, -1, I + 2)) * near_at(0, I + 2, -1)
                far = halo[side, away, pl.ds(TILE, I), :]
                outside = step(near_at(0), *pair(far, True), near_at(-1), near_at(1),
                               line(flows.at[0], outer, 0, I), line(flows.at[1], outer, 0, I))

                def here(di):
                    return reply[side, pl.ds(TILE + di, I), :]

                first = step(here(0), *pair(outside, False), here(-1), here(1),
                             line(flows.at[0], edge, 0, I), line(flows.at[1], edge, 0, I))
                then = (RATE + sign * line(flows.at[0], inner, 0, I)) * here(0)
                end[edge] = end[edge] + first
                end[inner] = end[inner] + then
                if side == LOWER:
                    spill[LOWER] = spill[LOWER] - first - then

    with jax.named_scope("sent"):
        one, two = exists[LOWER], exists[UPPER]
        for has, cells, slanted in ((later, 7 * I + 12, 10), (jnp.logical_not(later), 7 * I + 18, 0)):
            for many, number in ((one != two, 1), (one & two, 2)):
                @pl.when(has & many)
                def _(cells=cells, slanted=slanted, number=number):
                    count(load_sem.at[0], number * cells)
                    if slanted:
                        count(load_sem.at[3], number * slanted)
        sooner = ((lax.rem(e, 2) == 0) & exists[RIGHT]) | ((lax.rem(e, 2) == 1) & exists[LEFT])
        pl.when(sooner & later)(lambda: count(load_sem.at[1], 20 * (J + 1)))
        pl.when(sooner & jnp.logical_not(later))(lambda: count(load_sem.at[1], 10 * (J + 2)))
        pl.when(later & jnp.logical_not(sooner))(lambda: count(load_sem.at[1], 10 * J))
    with jax.named_scope("take"):
        for given in range(1, souths):
            piece = totals.at[pl.ds(0, given)]
            pl.when(s == given)(lambda piece=piece: pltpu.make_async_copy(piece, piece, total_recv).wait())
        before[...] = lax.fori_loop(0, s, lambda source, state: state + totals[source], spill[LOWER])
    for given in range(1, souths):
        piece = totals.at[pl.ds(0, given)]
        pl.when(s == souths - 1 - given)(lambda piece=piece: pltpu.make_async_copy(piece, piece, load_sem.at[2]).wait())


def write_out(scale, before, end, running_out, end_out, running, sems):
    J = end.shape[0]
    parts = 2 if J % 2 == 0 else 1
    rows = J // parts
    copies = [pltpu.make_async_copy(end, end_out, sems.at[0])]
    copies[0].start()
    state = before[...]
    for part in range(parts):
        for row in range(part * rows, (part + 1) * rows):
            state = state + end[row]
            running[row] = state * scale
        area = pl.ds(part * rows, rows)
        copies.append(pltpu.make_async_copy(running.at[area], running_out.at[area], sems.at[1 + part]))
        copies[-1].start()
    for copy in copies:
        copy.wait()


def per_device(souths, easts, tracer, flow_j, flow_i):
    J, I, M = tracer.shape
    out = jax.ShapeDtypeStruct((J, I, M), jnp.float32)
    padded = (J + 2 * PAD, I + 2 * TILE, M)
    dma = pltpu.SemaphoreType.DMA
    results = pl.pallas_call(
        functools.partial(kernel, souths, easts),
        out_shape=(jax.ShapeDtypeStruct((I, M), jnp.float32), out),
        in_specs=[pl.BlockSpec(memory_space=pl.ANY)] * 3,
        out_specs=(pl.BlockSpec(memory_space=pltpu.VMEM),) * 2,
        scratch_shapes=[pltpu.VMEM(padded, jnp.float32)] * 4
        + [
            pltpu.VMEM((2,) + padded, jnp.float32),
            pltpu.VMEM((2, 2) + padded[1:], jnp.float32),
            pltpu.VMEM((2,) + padded[1:], jnp.float32),
            pltpu.VMEM((2, I, M), jnp.float32),
            pltpu.VMEM((2,) + padded[1:], jnp.float32),
            pltpu.VMEM((2, 2, 2, TILE, M), jnp.float32),
            pltpu.VMEM((2, 2, 2, TILE, M), jnp.float32),
            pltpu.VMEM((2,) + padded[1:], jnp.float32),
            pltpu.VMEM((2, 2, TILE, M), jnp.float32),
            pltpu.VMEM((max(20 * (J + 2), 14 * I + 40), M), jnp.float32),
            pltpu.VMEM((I, M), jnp.float32),
            pltpu.VMEM((souths, I, M), jnp.float32),
            pltpu.SemaphoreType.REGULAR((max(1, (souths - 1).bit_length()),)),
            dma((4,)), dma((2,)), dma((2,)), dma((2,)), dma((2,)), dma((2,)), dma, dma((2,)), pltpu.SemaphoreType.REGULAR,
        ],
        compiler_params=pltpu.CompilerParams(collective_id=0, has_side_effects=True,
                                             vmem_limit_bytes=106 * 2 ** 19),
    )(tracer, flow_j, flow_i)
    return pl.pallas_call(
        functools.partial(write_out, 1.0 / (J * souths)),
        out_shape=(out, out),
        in_specs=[pl.BlockSpec(memory_space=pltpu.VMEM)] * 2,
        out_specs=(pl.BlockSpec(memory_space=pl.ANY),) * 2,
        scratch_shapes=[pltpu.VMEM((J, I, M), jnp.float32), pltpu.SemaphoreType.DMA((3,))],
        compiler_params=pltpu.CompilerParams(vmem_limit_bytes=2 ** 21),
    )(*results)


def solution(mesh):
    spec = P("south", "east", None)
    body = functools.partial(per_device, mesh.shape["south"], mesh.shape["east"])
    return jax.shard_map(body, mesh=mesh, in_specs=(spec,) * 3, out_specs=(spec,) * 2, check_vma=False)
```

```python
import functools

import jax
import jax.numpy as jnp
from jax import lax
from jax.experimental import pallas as pl
from jax.experimental.pallas import tpu as pltpu
from jax.sharding import PartitionSpec as P

RATE = 0.05
PAD = 2
TILE = 8
MESH = pl.DeviceIdType.MESH
LOWER, UPPER, LEFT, RIGHT = range(4)
SIDES = ((-1, 0), (1, 0), (0, -1), (0, 1))
BACK = (UPPER, LOWER, RIGHT, LEFT)


def chunk_of(rows, most):
    return max(c for c in range(1, most + 1) if rows % c == 0)


def view(ref, row, rows, col, cols):
    return ref.at[pl.ds(row + PAD, rows), pl.ds(col + TILE, cols), :]


def line(ref, row, col, cols):
    return ref[row + PAD, pl.ds(col + TILE, cols), :]


def step(middle, lower_j, upper_j, lower_i, upper_i, flow_j, flow_i):
    spread = lower_j + upper_j + lower_i + upper_i - 4.0 * middle
    return middle - flow_j * (upper_j - lower_j) - flow_i * (upper_i - lower_i) + RATE * spread


def advance(level, flows, row, rows, col, cols):
    def at(dj, di):
        return view(level, row + dj, rows, col + di, cols)[...]

    return step(at(0, 0), at(-1, 0), at(1, 0), at(0, -1), at(0, 1),
                view(flows.at[0], row, rows, col, cols)[...], view(flows.at[1], row, rows, col, cols)[...])


def kernel(souths, easts, tracer, flow_j, flow_i, before, end, level0, level1, level2, level3, flows, halo, reply, spill,
           part, tracer_bits, flow_bits, mine, mine_bits, tally, own, totals, ready, load_sem, bits_sem, side_sem, far_sem, last_sem,
           step_sem, total_recv, diag_sem, greeted):
    J, I, M = tracer.shape
    s, e = lax.axis_index("south"), lax.axis_index("east")
    levels = (level0, level1, level2, level3)
    zeros = functools.partial(jnp.zeros, dtype=jnp.float32)
    exists = (s > 0, s < souths - 1, e > 0, e < easts - 1)

    def peer(side):
        return {"south": s + SIDES[side][0], "east": e + SIDES[side][1]}

    barrier = pltpu.get_barrier_semaphore()
    near = 0
    for side in range(4):
        near = near + exists[side].astype(jnp.int32)

        @pl.when(exists[side])
        def _(side=side):
            pl.semaphore_signal(barrier, inc=1, device_id=peer(side), device_id_type=MESH)

    fields = ((tracer, level0), (flow_j, flows.at[0]), (flow_i, flows.at[1]))
    for number, some, spans in ((0, fields[:1], ((0, 2), (J - 2, 2))), (1, fields[1:], ((0, 2), (J - 2, 2))),
                                (2, fields[:1], ((2, J - 4),)), (3, fields[1:], ((2, J - 4),))):
        for src, dst in some:
            for row, rows in spans:
                pltpu.make_async_copy(src.at[pl.ds(row, rows)], view(dst, row, rows, 0, I), load_sem.at[number]).start()

    stages, known = [], 1
    while known < souths - 1:
        stages.append(known)
        known *= 2

    def tell(stage):
        reach = stages[stage]
        for ok, other in ((s >= reach, s - reach), (s + reach < souths, s + reach)):
            @pl.when(ok)
            def _(other=other):
                pl.semaphore_signal(ready.at[stage], inc=1, device_id={"south": other, "east": e}, device_id_type=MESH)

    def hear(stage):
        reach = stages[stage]
        pl.semaphore_wait(ready.at[stage], (s >= reach).astype(jnp.int32) + (s + reach < souths).astype(jnp.int32))

    def clear(level, row, rows, col, cols):
        view(level, row, rows, col, cols)[...] = zeros((rows, cols, M))

    def trim(k, row, rows, wide, sides=(LEFT, RIGHT)):
        for side in sides:
            col = {LEFT: -wide, RIGHT: I}[side]
            pl.when(jnp.logical_not(exists[side]))(lambda col=col: clear(levels[k], row, rows, col, wide))

    with jax.named_scope("clear"):
        clear(level2, -2, 2, -2, I + 4)
        clear(level2, J, 2, -2, I + 4)
        clear(level3, -2, 1, 0, I)
        clear(level3, J + 1, 1, 0, I)
        spill[...] = zeros(spill.shape)
        for side, row in ((LOWER, -1), (UPPER, J)):
            pl.when(jnp.logical_not(exists[side]))(lambda row=row: clear(level0, row, 1, -3, I + 6))
        trim(0, 0, J, 4)
        for side in (LEFT, RIGHT):
            @pl.when(jnp.logical_not(exists[side]))
            def _(side=side):
                tracer_bits[side - LEFT, :, :, pl.ds((0, 2)[side - LEFT], 3), :] = zeros((2, 2, 3, M))
    with jax.named_scope("barw"):
        pl.semaphore_wait(barrier, near)
        for turn, late in enumerate((LEFT, RIGHT)):
            @pl.when((lax.rem(e, 2) == turn) & exists[late])
            def _(late=late):
                pl.semaphore_signal(greeted, inc=1, device_id=peer(late), device_id_type=MESH)
    later = ((lax.rem(e, 2) == 0) & exists[LEFT]) | ((lax.rem(e, 2) == 1) & exists[RIGHT])

    def remote(side, src, dst, send, recv):
        return pltpu.make_async_remote_copy(src_ref=src, dst_ref=dst, send_sem=send, recv_sem=recv,
                                            device_id=peer(side), device_id_type=MESH)

    def block(ref, side, at_home, row, rows, col, cols):
        if side in (LOWER, UPPER):
            row = {(LOWER, True): row, (LOWER, False): J + row,
                   (UPPER, True): J - row - rows, (UPPER, False): -row - rows}[side, at_home]
        else:
            col = {(LEFT, True): col, (LEFT, False): I + col,
                   (RIGHT, True): I - col - cols, (RIGHT, False): -col - cols}[side, at_home]
        if len(ref.shape) == 4:
            return ref.at[:, pl.ds(row + PAD, rows), pl.ds(col + TILE, cols), :]
        return view(ref, row, rows, col, cols)

    def shift(side, ref, sems, *area):
        return remote(side, block(ref, side, True, *area), block(ref, side, False, *area), load_sem.at[side // 2], sems.at[side % (2 if sems is side_sem else 4)])

    def far_tracer(side):
        return [shift(side, level0, far_sem, 0, 1, 0, I)]

    def far_flow(side):
        return [shift(side, flows.at[0], far_sem, 0, 1, 0, I)]

    def far_part(side):
        area = pl.ds(TILE + 1, I - 2)
        return [remote(side, mine.at[side, area, :], part.at[BACK[side], area, :], load_sem.at[side // 2], far_sem.at[side])]

    def far_last(side):
        return [shift(side, flows.at[1], last_sem, 0, 1, 0, I), shift(side, flows.at[0], last_sem, 1, 1, 0, I)]

    def side_tracer(side):
        return [shift(side, level0, side_sem, 0, J, 0, 4)]

    def side_flows(side):
        return [shift(side, flows, side_sem, 0, J, 0, 3)]

    bands = (LOWER, UPPER)

    edge, nearest = (0, J - 1), (0, 1)

    def bits(side):
        out = []
        to = BACK[side] - LEFT
        for band in bands:
            three, two = {LEFT: (0, 0), RIGHT: (I - 3, I - 2)}[side]
            out += [remote(side, view(level0, (0, J - 2)[band], 2, three, 3),
                           tracer_bits.at[to, band, :, pl.ds((0, 2)[to], 3), :], load_sem.at[side // 2], bits_sem.at[to]),
                    remote(side, flows.at[:, edge[band] + PAD, pl.ds(two + TILE, 2), :],
                           flow_bits.at[to, band, :, pl.ds((0, 1)[to], 2), :], load_sem.at[side // 2], bits_sem.at[to])]
        return out

    def own_bits():
        for to, own_tracer, own_flow in ((0, (3, 0), (2, 0)), (1, (0, I - 2), (0, I - 1))):
            for band in bands:
                tracer_bits[to, band, :, pl.ds(own_tracer[0], 2), :] = view(level0, (0, J - 2)[band], 2, own_tracer[1], 2)[...]
                flow_bits[to, band, :, pl.ds(own_flow[0], 1), :] = flows[:, edge[band] + PAD, pl.ds(own_flow[1] + TILE, 1), :]

    def lone(band, middle, inside, left, right, flow_j, flow_i):
        none = jnp.zeros_like(middle)
        lower, upper = (none, inside) if band == LOWER else (inside, none)
        return step(middle, lower, upper, left, right, flow_j, flow_i)

    def relay(band, side):
        to = side - LEFT
        row = (J, -1)[band] + PAD
        three, two, parts = ((-3, -2, -2), (I, I, I - 1))[to]

        def cells(src, dst, sem):
            return remote(band, src, dst, load_sem.at[0], sem.at[band])

        return [cells(tracer_bits.at[to, band, nearest[band], pl.ds((0, 2)[to], 3), :],
                      level0.at[row, pl.ds(three + TILE, 3), :], far_sem),
                cells(mine_bits.at[to, band, pl.ds(0, 3), :], part.at[BACK[band], pl.ds(parts + TILE, 3), :], far_sem),
                cells(flow_bits.at[to, band, 0, pl.ds((0, 1)[to], 2), :], flows.at[0, row, pl.ds(two + TILE, 2), :], far_sem)]

    def cell(band, side):
        area = pl.ds({LEFT: 0, RIGHT: I - 1}[side] + TILE, 1)
        row = (J + 1, -2)[band] + PAD
        return [remote(band, level0.at[(1, J - 2)[band] + PAD, area, :], level0.at[row, area, :], load_sem.at[0], far_sem.at[band]),
                remote(band, flows.at[1, edge[band] + PAD, area, :], flows.at[1, row, area, :], load_sem.at[0], far_sem.at[band])]

    def diagonal(band, side):
        row = (J, -1)[band] + PAD, (J + 1, -2)[band] + PAD
        home, away = {LEFT: ((0, 0), (I, I)), RIGHT: ((I - 3, I - 2), (-3, -2))}[side]

        def cells(src, dst):
            return pltpu.make_async_remote_copy(
                src_ref=src, dst_ref=dst, send_sem=load_sem.at[3], recv_sem=diag_sem.at[band],
                device_id={"south": s + SIDES[band][0], "east": e + SIDES[side][1]}, device_id_type=MESH)

        return [cells(view(level0, (0, J - 2)[band], 2, home[0], 3), view(level0, (J, -2)[band], 2, away[0], 3))] + [
            cells(flows.at[k, edge[band] + PAD, pl.ds(home[1] + TILE, 2), :], flows.at[k, row[k], pl.ds(away[1] + TILE, 2), :])
            for k in (0, 1)]

    def second(side):
        row = {LOWER: 0, UPPER: J - 2}[side]
        return remote(side, view(level2, row, 2, -1, I + 2), halo.at[BACK[side], :, pl.ds(TILE - 1, I + 2), :],
                      load_sem.at[0], step_sem.at[side])

    def start(side, make):
        @pl.when(exists[side])
        def _():
            for copy in make():
                copy.start()

    def count(sem, cells):
        area = tally.at[pl.ds(0, cells)]
        pltpu.make_async_copy(area, area, sem).wait()

    def drain(sem, rows, cols, ref=None):
        part = (level0 if ref is None else ref).at[..., pl.ds(0, rows), pl.ds(0, cols), :]
        pltpu.make_async_copy(part, part, sem).wait()

    def update(k, row, rows, col, cols):
        value = advance(levels[k - 1], flows, row, rows, col, cols)
        if k == 4:
            end[pl.ds(row, rows), pl.ds(col, cols), :] = value
        else:
            view(levels[k], row, rows, col, cols)[...] = value

    def sweep(k, first, last, col, cols, most):
        rows = chunk_of(last - first, most)

        def body(turn, _):
            update(k, first + turn * rows, rows, col, cols)
            return 0

        lax.fori_loop(0, (last - first) // rows, body, 0)

    def both(*makes, sides=(LOWER, UPPER)):
        for turn in range(2):
            @pl.when(lax.rem(s, 2) == turn)
            def _(turn=turn):
                for side in (sides if turn == 0 else sides[::-1]):
                    start(side, lambda side=side: [copy for make in makes for copy in make(side)])

    def share(side):
        to = side - LEFT
        pl.when(exists[side])(lambda: count(bits_sem.at[to], 20))
        for band in bands:
            def at(near, col):
                return tracer_bits[to, band, nearest[band] if near else 1 - nearest[band], pl.ds(col, 3), :]

            mine_bits[to, band, pl.ds(0, 3), :] = lone(band, at(True, 1), at(False, 1), at(True, 0), at(True, 2),
                                                       flow_bits[to, band, 0, pl.ds(0, 3), :],
                                                       flow_bits[to, band, 1, pl.ds(0, 3), :])
        for band in bands:
            start(band, lambda band=band: relay(band, side))

    def strip(side):
        pl.when(exists[side])(lambda: drain(side_sem.at[BACK[side] % 2], J, 10))
        for k in range(1, 5):
            sweep(k, k, J - k, {LEFT: k - 4, RIGHT: I - k}[side], 4, 15)
            if k < 4:
                trim(k, k, J - 2 * k, 4 - k, (side,))

    with jax.named_scope("load0"):
        drain(load_sem.at[0], 4, I)
        both(far_tracer)
    with jax.named_scope("load1"):
        drain(load_sem.at[1], 4, I, flows)
        for turn, (early, late) in enumerate(((RIGHT, LEFT), (LEFT, RIGHT))):
            @pl.when(lax.rem(e, 2) == turn)
            def _(early=early, late=late):
                start(early, lambda: bits(early))

                @pl.when(exists[late])
                def _():
                    for band in bands:
                        start(band, lambda band=band: cell(band, late))
        both(far_flow)
        for band in bands:
            row, inside = edge[band], (1, J - 2)[band]
            mine[band, pl.ds(TILE + 1, I - 2), :] = lone(
                band, *(line(level0, r, c, I - 2) for r, c in ((row, 1), (inside, 1), (row, 0), (row, 2))),
                *(line(flows.at[k], row, 1, I - 2) for k in (0, 1)))
        own_bits()
        both(far_part)
        if stages:
            tell(0)
    with jax.named_scope("load2"):
        drain(load_sem.at[2], J - 4, I)
        for side in (LEFT, RIGHT):
            start(side, lambda side=side: side_tracer(side))
    with jax.named_scope("load3"):
        drain(load_sem.at[3], J - 4, I, flows)
        for side in (LEFT, RIGHT):
            start(side, lambda side=side: side_flows(side))
    with jax.named_scope("inner"):
        for k in range(1, 5):
            sweep(k, k, J - k, k, I - 2 * k, 7)
    def greet():
        for stage in range(1, len(stages) - 1):
            hear(stage - 1)
            tell(stage)

    for turn, (early, late) in enumerate(((RIGHT, LEFT), (LEFT, RIGHT))):
        @pl.when(lax.rem(e, 2) == turn)
        def _(early=early, late=late):
            with jax.named_scope("diag"):
                @pl.when(exists[late])
                def _():
                    pl.semaphore_wait(greeted, 1)
                    for band in bands:
                        start(band, lambda band=band: diagonal(band, late))
            with jax.named_scope("hearx"):
                pl.when(2 * e >= easts)(greet)
            with jax.named_scope("early"):
                share(early)
                pl.when(jnp.logical_not(exists[late]))(lambda: share(late))
                strip(early)
                both(far_last)
            with jax.named_scope("hear0"):
                pl.when(2 * e < easts)(greet)
            with jax.named_scope("hear1"):
                for stage in range(max(1, len(stages) - 1), len(stages)):
                    hear(stage - 1)
                    tell(stage)
            with jax.named_scope("late"):
                strip(late)
    total = end[4]
    for row in range(5, J - 4):
        total = total + end[row]

    def rim(side):
        edge_row, outer, two, three, four, sign = ((0, -1, 0, 0, 0, -1.0), (J - 1, J, J - 2, J - 3, J - 4, 1.0))[side]
        pl.when(exists[side] & jnp.logical_not(later))(lambda: count(far_sem.at[BACK[side]], 3 * I + 14))

        @pl.when(exists[side] & later)
        def _():
            count(far_sem.at[BACK[side]], 3 * I + 8)
            count(diag_sem.at[BACK[side]], 10)
        beyond = outer + outer - edge_row
        for turn, col in enumerate((-2, I - 1)):
            @pl.when((lax.rem(e, 2) == turn) & exists[side] & later)
            def _(col=col):
                part[side, pl.ds(TILE + col, 3), :] = lone(
                    BACK[side], *(line(level0, r, c, 3) for r, c in
                                  ((outer, col), (beyond, col), (outer, col - 1), (outer, col + 1))),
                    line(flows.at[0], outer, col, 3), line(flows.at[1], beyond, col, 3))
        update(1, edge_row, 1, -3, I + 6)
        trim(1, edge_row, 1, 3)
        level1[outer + PAD, pl.ds(TILE - 2, I + 4), :] = part[side, pl.ds(TILE - 2, I + 4), :] + (
            RATE + sign * line(flows.at[0], outer, -2, I + 4)) * line(level0, edge_row, -2, I + 4)
        trim(1, outer, 1, 2)
        pl.when(jnp.logical_not(exists[side]))(lambda: clear(level1, outer, 1, -2, I + 4))
        update(2, two, 2, -2, I + 4)
        trim(2, two, 2, 2)
        start(side, lambda: [second(side)])
        update(3, three, 3, -1, I + 2)
        trim(3, three, 3, 1)
        level3[outer + PAD, pl.ds(TILE - 1, I + 2), :] = zeros((I + 2, M))

        @pl.when(exists[side])
        def _():
            level3[outer + PAD, pl.ds(TILE - 1, I + 2), :] = (
                RATE + sign * line(flows.at[0], outer, -1, I + 2)) * line(level2, edge_row, -1, I + 2)

        trim(3, outer, 1, 1)
        update(4, four, 4, 0, I)

    for turn, sides in enumerate(((LOWER, UPPER), (UPPER, LOWER))):
        @pl.when(lax.rem(s, 2) == turn)
        def _(sides=sides):
            for number, side in enumerate(sides):
                with jax.named_scope(f"rim{number}"):
                    rim(side)
    for row in (*range(4), *range(J - 4, J)):
        total = total + end[row]
    with jax.named_scope("spill"):
        for side, outer, last, sign in ((LOWER, -1, -2, -1.0), (UPPER, J, J + 1, 1.0)):
            @pl.when(exists[side])
            def _(side=side, outer=outer, last=last, sign=sign):
                count(last_sem.at[BACK[side]], 2 * I)
                value = advance(level3, flows, outer, 1, 0, I)[0]
                spill[side] = value + (RATE + sign * line(flows.at[0], last, 0, I)) * line(level3, outer, 0, I)

        own[...] = total + spill[LOWER] + spill[UPPER]

    def total_copy(source, other):
        return pltpu.make_async_remote_copy(
            src_ref=own, dst_ref=totals.at[source], send_sem=load_sem.at[2], recv_sem=total_recv,
            device_id={"south": other, "east": e}, device_id_type=MESH)

    with jax.named_scope("give"):
        reach = stages[-1] if stages else souths
        odd, even = (souths - s) // 2, (souths - s - 1) // 2
        near_odd, near_even = jnp.minimum(odd, (reach + 1) // 2), jnp.minimum(even, reach // 2)

        def give(lower, upper, distance):
            def one(turn, _):
                total_copy(s, s + distance(turn)).start()
                return 0

            lax.fori_loop(lower, upper, one, 0)

        give(0, near_odd, lambda turn: 2 * turn + 1)
        give(0, near_even, lambda turn: 2 * (near_even - turn))
        if stages:
            hear(len(stages) - 1)
            give(near_odd, odd, lambda turn: 2 * turn + 1)
            give(0, even - near_even, lambda turn: 2 * (even - turn))

    with jax.named_scope("recv2"):
        for side in (LOWER, UPPER):
            pl.when(exists[side])(lambda side=side: second(BACK[side]).wait_recv())
    with jax.named_scope("reply"):
        for side, sign, edge, inner, outer, close, away in (
            (LOWER, 1.0, 0, 1, -1, 1, 0), (UPPER, -1.0, J - 1, J - 2, J, 0, 1),
        ):
            @pl.when(exists[side])
            def _(side=side, sign=sign, edge=edge, inner=inner, outer=outer, close=close, away=away):
                def near_at(di, cols=I, col=0):
                    return halo[side, close, pl.ds(TILE + col + di, cols), :]

                def pair(value, at_outer):
                    none = jnp.zeros_like(value)
                    lower = (side == LOWER)
                    return (value, none) if lower else (none, value)

                reply[side, pl.ds(TILE - 1, I + 2), :] = (
                    RATE + sign * line(flows.at[0], edge, -1, I + 2)) * near_at(0, I + 2, -1)
                far = halo[side, away, pl.ds(TILE, I), :]
                outside = step(near_at(0), *pair(far, True), near_at(-1), near_at(1),
                               line(flows.at[0], outer, 0, I), line(flows.at[1], outer, 0, I))

                def here(di):
                    return reply[side, pl.ds(TILE + di, I), :]

                first = step(here(0), *pair(outside, False), here(-1), here(1),
                             line(flows.at[0], edge, 0, I), line(flows.at[1], edge, 0, I))
                then = (RATE + sign * line(flows.at[0], inner, 0, I)) * here(0)
                end[edge] = end[edge] + first
                end[inner] = end[inner] + then
                if side == LOWER:
                    spill[LOWER] = spill[LOWER] - first - then

    with jax.named_scope("sent"):
        one, two = exists[LOWER], exists[UPPER]
        for has, cells, slanted in ((later, 7 * I + 12, 10), (jnp.logical_not(later), 7 * I + 18, 0)):
            for many, number in ((one != two, 1), (one & two, 2)):
                @pl.when(has & many)
                def _(cells=cells, slanted=slanted, number=number):
                    count(load_sem.at[0], number * cells)
                    if slanted:
                        count(load_sem.at[3], number * slanted)
        sooner = ((lax.rem(e, 2) == 0) & exists[RIGHT]) | ((lax.rem(e, 2) == 1) & exists[LEFT])
        pl.when(sooner & later)(lambda: count(load_sem.at[1], 20 * (J + 1)))
        pl.when(sooner & jnp.logical_not(later))(lambda: count(load_sem.at[1], 10 * (J + 2)))
        pl.when(later & jnp.logical_not(sooner))(lambda: count(load_sem.at[1], 10 * J))
    with jax.named_scope("take"):
        for given in range(1, souths):
            piece = totals.at[pl.ds(0, given)]
            pl.when(s == given)(lambda piece=piece: pltpu.make_async_copy(piece, piece, total_recv).wait())
        before[...] = lax.fori_loop(0, s, lambda source, state: state + totals[source], spill[LOWER])
    for given in range(1, souths):
        piece = totals.at[pl.ds(0, given)]
        pl.when(s == souths - 1 - given)(lambda piece=piece: pltpu.make_async_copy(piece, piece, load_sem.at[2]).wait())


def write_out(scale, before, end, running_out, end_out, running, sems):
    J = end.shape[0]
    parts = 2 if J % 2 == 0 else 1
    rows = J // parts
    copies = [pltpu.make_async_copy(end, end_out, sems.at[0])]
    copies[0].start()
    state = before[...]
    for part in range(parts):
        for row in range(part * rows, (part + 1) * rows):
            state = state + end[row]
            running[row] = state * scale
        area = pl.ds(part * rows, rows)
        copies.append(pltpu.make_async_copy(running.at[area], running_out.at[area], sems.at[1 + part]))
        copies[-1].start()
    for copy in copies:
        copy.wait()


def per_device(souths, easts, tracer, flow_j, flow_i):
    J, I, M = tracer.shape
    out = jax.ShapeDtypeStruct((J, I, M), jnp.float32)
    padded = (J + 2 * PAD, I + 2 * TILE, M)
    dma = pltpu.SemaphoreType.DMA
    results = pl.pallas_call(
        functools.partial(kernel, souths, easts),
        out_shape=(jax.ShapeDtypeStruct((I, M), jnp.float32), out),
        in_specs=[pl.BlockSpec(memory_space=pl.ANY)] * 3,
        out_specs=(pl.BlockSpec(memory_space=pltpu.VMEM),) * 2,
        scratch_shapes=[pltpu.VMEM(padded, jnp.float32)] * 4
        + [
            pltpu.VMEM((2,) + padded, jnp.float32),
            pltpu.VMEM((2, 2) + padded[1:], jnp.float32),
            pltpu.VMEM((2,) + padded[1:], jnp.float32),
            pltpu.VMEM((2, I, M), jnp.float32),
            pltpu.VMEM((2,) + padded[1:], jnp.float32),
            pltpu.VMEM((2, 2, 2, TILE, M), jnp.float32),
            pltpu.VMEM((2, 2, 2, TILE, M), jnp.float32),
            pltpu.VMEM((2,) + padded[1:], jnp.float32),
            pltpu.VMEM((2, 2, TILE, M), jnp.float32),
            pltpu.VMEM((max(20 * (J + 2), 14 * I + 40), M), jnp.float32),
            pltpu.VMEM((I, M), jnp.float32),
            pltpu.VMEM((souths, I, M), jnp.float32),
            pltpu.SemaphoreType.REGULAR((max(1, (souths - 1).bit_length()),)),
            dma((4,)), dma((2,)), dma((2,)), dma((2,)), dma((2,)), dma((2,)), dma, dma((2,)), pltpu.SemaphoreType.REGULAR,
        ],
        compiler_params=pltpu.CompilerParams(collective_id=0, has_side_effects=True,
                                             vmem_limit_bytes=106 * 2 ** 19),
    )(tracer, flow_j, flow_i)
    return pl.pallas_call(
        functools.partial(write_out, 1.0 / (J * souths)),
        out_shape=(out, out),
        in_specs=[pl.BlockSpec(memory_space=pltpu.VMEM)] * 2,
        out_specs=(pl.BlockSpec(memory_space=pl.ANY),) * 2,
        scratch_shapes=[pltpu.VMEM((J, I, M), jnp.float32), pltpu.SemaphoreType.DMA((3,))],
        compiler_params=pltpu.CompilerParams(vmem_limit_bytes=2 ** 21),
    )(*results)


def solution(mesh):
    spec = P("south", "east", None)
    body = functools.partial(per_device, mesh.shape["south"], mesh.shape["east"])
    return jax.shard_map(body, mesh=mesh, in_specs=(spec,) * 3, out_specs=(spec,) * 2, check_vma=False)
```

```python
import functools

import jax
import jax.numpy as jnp
from jax import lax
from jax.experimental import pallas as pl
from jax.experimental.pallas import tpu as pltpu
from jax.sharding import PartitionSpec as P

RATE = 0.05
PAD = 2
TILE = 8
MESH = pl.DeviceIdType.MESH
LOWER, UPPER, LEFT, RIGHT = range(4)
SIDES = ((-1, 0), (1, 0), (0, -1), (0, 1))
BACK = (UPPER, LOWER, RIGHT, LEFT)


def chunk_of(rows, most):
    return max(c for c in range(1, most + 1) if rows % c == 0)


def view(ref, row, rows, col, cols):
    return ref.at[pl.ds(row + PAD, rows), pl.ds(col + TILE, cols), :]


def line(ref, row, col, cols):
    return ref[row + PAD, pl.ds(col + TILE, cols), :]


def step(middle, lower_j, upper_j, lower_i, upper_i, flow_j, flow_i):
    spread = lower_j + upper_j + lower_i + upper_i - 4.0 * middle
    return middle - flow_j * (upper_j - lower_j) - flow_i * (upper_i - lower_i) + RATE * spread


def advance(level, flows, row, rows, col, cols):
    def at(dj, di):
        return view(level, row + dj, rows, col + di, cols)[...]

    return step(at(0, 0), at(-1, 0), at(1, 0), at(0, -1), at(0, 1),
                view(flows.at[0], row, rows, col, cols)[...], view(flows.at[1], row, rows, col, cols)[...])


def kernel(souths, easts, tracer, flow_j, flow_i, before, end, level0, level1, level2, level3, flows, halo, reply, spill,
           part, tracer_bits, flow_bits, mine, mine_bits, tally, own, totals, ready, load_sem, bits_sem, side_sem, far_sem, last_sem,
           step_sem, total_recv, greeted):
    J, I, M = tracer.shape
    s, e = lax.axis_index("south"), lax.axis_index("east")
    levels = (level0, level1, level2, level3)
    zeros = functools.partial(jnp.zeros, dtype=jnp.float32)
    exists = (s > 0, s < souths - 1, e > 0, e < easts - 1)

    def peer(side):
        return {"south": s + SIDES[side][0], "east": e + SIDES[side][1]}

    barrier = pltpu.get_barrier_semaphore()
    near = 0
    for side in range(4):
        near = near + exists[side].astype(jnp.int32)

        @pl.when(exists[side])
        def _(side=side):
            pl.semaphore_signal(barrier, inc=1, device_id=peer(side), device_id_type=MESH)

    fields = ((tracer, level0), (flow_j, flows.at[0]), (flow_i, flows.at[1]))
    for number, some, spans in ((0, fields[:1], ((0, 2), (J - 2, 2))), (1, fields[1:], ((0, 2), (J - 2, 2))),
                                (2, fields[:1], ((2, J - 4),)), (3, fields[1:], ((2, J - 4),))):
        for src, dst in some:
            for row, rows in spans:
                pltpu.make_async_copy(src.at[pl.ds(row, rows)], view(dst, row, rows, 0, I), load_sem.at[number]).start()

    stages, known = [], 1
    while known < souths - 1:
        stages.append(known)
        known *= 2

    def tell(stage):
        reach = stages[stage]
        for ok, other in ((s >= reach, s - reach), (s + reach < souths, s + reach)):
            @pl.when(ok)
            def _(other=other):
                pl.semaphore_signal(ready.at[stage], inc=1, device_id={"south": other, "east": e}, device_id_type=MESH)

    def hear(stage):
        reach = stages[stage]
        pl.semaphore_wait(ready.at[stage], (s >= reach).astype(jnp.int32) + (s + reach < souths).astype(jnp.int32))

    def clear(level, row, rows, col, cols):
        view(level, row, rows, col, cols)[...] = zeros((rows, cols, M))

    def trim(k, row, rows, wide, sides=(LEFT, RIGHT)):
        for side in sides:
            col = {LEFT: -wide, RIGHT: I}[side]
            pl.when(jnp.logical_not(exists[side]))(lambda col=col: clear(levels[k], row, rows, col, wide))

    with jax.named_scope("clear"):
        clear(level2, -2, 2, -2, I + 4)
        clear(level2, J, 2, -2, I + 4)
        clear(level3, -2, 1, 0, I)
        clear(level3, J + 1, 1, 0, I)
        spill[...] = zeros(spill.shape)
        for side, row in ((LOWER, -1), (UPPER, J)):
            pl.when(jnp.logical_not(exists[side]))(lambda row=row: clear(level0, row, 1, -3, I + 6))
        trim(0, 0, J, 4)
        for side in (LEFT, RIGHT):
            @pl.when(jnp.logical_not(exists[side]))
            def _(side=side):
                tracer_bits[side - LEFT, :, :, pl.ds((0, 2)[side - LEFT], 3), :] = zeros((2, 2, 3, M))
    with jax.named_scope("barw"):
        pl.semaphore_wait(barrier, near)
        for turn, late in enumerate((LEFT, RIGHT)):
            @pl.when((lax.rem(e, 2) == turn) & exists[late])
            def _(late=late):
                pl.semaphore_signal(greeted, inc=1, device_id=peer(late), device_id_type=MESH)
    later = ((lax.rem(e, 2) == 0) & exists[LEFT]) | ((lax.rem(e, 2) == 1) & exists[RIGHT])

    def remote(side, src, dst, send, recv):
        return pltpu.make_async_remote_copy(src_ref=src, dst_ref=dst, send_sem=send, recv_sem=recv,
                                            device_id=peer(side), device_id_type=MESH)

    def block(ref, side, at_home, row, rows, col, cols):
        if side in (LOWER, UPPER):
            row = {(LOWER, True): row, (LOWER, False): J + row,
                   (UPPER, True): J - row - rows, (UPPER, False): -row - rows}[side, at_home]
        else:
            col = {(LEFT, True): col, (LEFT, False): I + col,
                   (RIGHT, True): I - col - cols, (RIGHT, False): -col - cols}[side, at_home]
        if len(ref.shape) == 4:
            return ref.at[:, pl.ds(row + PAD, rows), pl.ds(col + TILE, cols), :]
        return view(ref, row, rows, col, cols)

    def shift(side, ref, sems, *area):
        return remote(side, block(ref, side, True, *area), block(ref, side, False, *area), load_sem.at[side // 2], sems.at[side % (2 if sems is side_sem else 4)])

    def far_tracer(side):
        return [shift(side, level0, far_sem, 0, 1, 0, I)]

    def far_flow(side):
        return [shift(side, flows.at[0], far_sem, 0, 1, 0, I)]

    def far_part(side):
        area = pl.ds(TILE + 1, I - 2)
        return [remote(side, mine.at[side, area, :], part.at[BACK[side], area, :], load_sem.at[side // 2], far_sem.at[side])]

    def far_last(side):
        return [shift(side, flows.at[1], last_sem, 0, 1, 0, I), shift(side, flows.at[0], last_sem, 1, 1, 0, I)]

    def side_tracer(side):
        return [shift(side, level0, side_sem, 0, J, 0, 4)]

    def side_flows(side):
        return [shift(side, flows, side_sem, 0, J, 0, 3)]

    bands = (LOWER, UPPER)

    edge, nearest = (0, J - 1), (0, 1)

    def bits(side):
        out = []
        to = BACK[side] - LEFT
        for band in bands:
            three, two = {LEFT: (0, 0), RIGHT: (I - 3, I - 2)}[side]
            out += [remote(side, view(level0, (0, J - 2)[band], 2, three, 3),
                           tracer_bits.at[to, band, :, pl.ds((0, 2)[to], 3), :], load_sem.at[side // 2], bits_sem),
                    remote(side, flows.at[:, edge[band] + PAD, pl.ds(two + TILE, 2), :],
                           flow_bits.at[to, band, :, pl.ds((0, 1)[to], 2), :], load_sem.at[side // 2], bits_sem)]
        return out

    def own_bits():
        for to, own_tracer, own_flow in ((0, (3, 0), (2, 0)), (1, (0, I - 2), (0, I - 1))):
            for band in bands:
                tracer_bits[to, band, :, pl.ds(own_tracer[0], 2), :] = view(level0, (0, J - 2)[band], 2, own_tracer[1], 2)[...]
                flow_bits[to, band, :, pl.ds(own_flow[0], 1), :] = flows[:, edge[band] + PAD, pl.ds(own_flow[1] + TILE, 1), :]

    def lone(band, middle, inside, left, right, flow_j, flow_i):
        none = jnp.zeros_like(middle)
        lower, upper = (none, inside) if band == LOWER else (inside, none)
        return step(middle, lower, upper, left, right, flow_j, flow_i)

    def relay(band, side):
        to = side - LEFT
        row = (J, -1)[band] + PAD
        three, two, parts = ((-3, -2, -2), (I, I, I - 1))[to]

        def cells(src, dst, sem):
            return remote(band, src, dst, load_sem.at[0], sem.at[band])

        return [cells(tracer_bits.at[to, band, nearest[band], pl.ds((0, 2)[to], 3), :],
                      level0.at[row, pl.ds(three + TILE, 3), :], far_sem),
                cells(mine_bits.at[to, band, pl.ds(0, 3), :], part.at[BACK[band], pl.ds(parts + TILE, 3), :], far_sem),
                cells(flow_bits.at[to, band, 0, pl.ds((0, 1)[to], 2), :], flows.at[0, row, pl.ds(two + TILE, 2), :], far_sem)]

    def cell(band, side):
        area = pl.ds({LEFT: 0, RIGHT: I - 1}[side] + TILE, 1)
        row = (J + 1, -2)[band] + PAD
        return [remote(band, level0.at[(1, J - 2)[band] + PAD, area, :], level0.at[row, area, :], load_sem.at[0], far_sem.at[band]),
                remote(band, flows.at[1, edge[band] + PAD, area, :], flows.at[1, row, area, :], load_sem.at[0], far_sem.at[band])]

    def diagonal(band, side):
        row = (J, -1)[band] + PAD, (J + 1, -2)[band] + PAD
        home, away = {LEFT: ((0, 0), (I, I)), RIGHT: ((I - 3, I - 2), (-3, -2))}[side]

        def cells(src, dst):
            return pltpu.make_async_remote_copy(
                src_ref=src, dst_ref=dst, send_sem=load_sem.at[3], recv_sem=far_sem.at[band],
                device_id={"south": s + SIDES[band][0], "east": e + SIDES[side][1]}, device_id_type=MESH)

        return [cells(view(level0, (0, J - 2)[band], 2, home[0], 3), view(level0, (J, -2)[band], 2, away[0], 3))] + [
            cells(flows.at[k, edge[band] + PAD, pl.ds(home[1] + TILE, 2), :], flows.at[k, row[k], pl.ds(away[1] + TILE, 2), :])
            for k in (0, 1)]

    def second(side):
        row = {LOWER: 0, UPPER: J - 2}[side]
        return remote(side, view(level2, row, 2, -1, I + 2), halo.at[BACK[side], :, pl.ds(TILE - 1, I + 2), :],
                      load_sem.at[0], step_sem.at[side])

    def start(side, make):
        @pl.when(exists[side])
        def _():
            for copy in make():
                copy.start()

    def count(sem, cells):
        area = tally.at[pl.ds(0, cells)]
        pltpu.make_async_copy(area, area, sem).wait()

    def drain(sem, rows, cols, ref=None):
        part = (level0 if ref is None else ref).at[..., pl.ds(0, rows), pl.ds(0, cols), :]
        pltpu.make_async_copy(part, part, sem).wait()

    def update(k, row, rows, col, cols):
        value = advance(levels[k - 1], flows, row, rows, col, cols)
        if k == 4:
            end[pl.ds(row, rows), pl.ds(col, cols), :] = value
        else:
            view(levels[k], row, rows, col, cols)[...] = value

    def sweep(k, first, last, col, cols, most):
        rows = chunk_of(last - first, most)

        def body(turn, _):
            update(k, first + turn * rows, rows, col, cols)
            return 0

        lax.fori_loop(0, (last - first) // rows, body, 0)

    def both(*makes, sides=(LOWER, UPPER)):
        for turn in range(2):
            @pl.when(lax.rem(s, 2) == turn)
            def _(turn=turn):
                for side in (sides if turn == 0 else sides[::-1]):
                    start(side, lambda side=side: [copy for make in makes for copy in make(side)])

    def share(side):
        to = side - LEFT
        pl.when(exists[side])(lambda: count(bits_sem, 20))
        for band in bands:
            def at(near, col):
                return tracer_bits[to, band, nearest[band] if near else 1 - nearest[band], pl.ds(col, 3), :]

            mine_bits[to, band, pl.ds(0, 3), :] = lone(band, at(True, 1), at(False, 1), at(True, 0), at(True, 2),
                                                       flow_bits[to, band, 0, pl.ds(0, 3), :],
                                                       flow_bits[to, band, 1, pl.ds(0, 3), :])
        for band in bands:
            start(band, lambda band=band: relay(band, side))

    def strip(side):
        pl.when(exists[side])(lambda: drain(side_sem.at[BACK[side] % 2], J, 10))
        for k in range(1, 5):
            sweep(k, k, J - k, {LEFT: k - 4, RIGHT: I - k}[side], 4, 15)
            if k < 4:
                trim(k, k, J - 2 * k, 4 - k, (side,))

    with jax.named_scope("load0"):
        drain(load_sem.at[0], 4, I)
        both(far_tracer)
    with jax.named_scope("load1"):
        drain(load_sem.at[1], 4, I, flows)
        for turn, (early, late) in enumerate(((RIGHT, LEFT), (LEFT, RIGHT))):
            @pl.when(lax.rem(e, 2) == turn)
            def _(early=early, late=late):
                start(early, lambda: bits(early))

                @pl.when(exists[late])
                def _():
                    for band in bands:
                        start(band, lambda band=band: cell(band, late))
        both(far_flow)
        for band in bands:
            row, inside = edge[band], (1, J - 2)[band]
            mine[band, pl.ds(TILE + 1, I - 2), :] = lone(
                band, *(line(level0, r, c, I - 2) for r, c in ((row, 1), (inside, 1), (row, 0), (row, 2))),
                *(line(flows.at[k], row, 1, I - 2) for k in (0, 1)))
        own_bits()
        both(far_part)
        if stages:
            tell(0)
    with jax.named_scope("load2"):
        drain(load_sem.at[2], J - 4, I)
        for side in (LEFT, RIGHT):
            start(side, lambda side=side: side_tracer(side))
    with jax.named_scope("load3"):
        drain(load_sem.at[3], J - 4, I, flows)
        for side in (LEFT, RIGHT):
            start(side, lambda side=side: side_flows(side))
    with jax.named_scope("inner"):
        for k in range(1, 5):
            sweep(k, k, J - k, k, I - 2 * k, 7)
    def greet():
        for stage in range(1, len(stages) - 1):
            hear(stage - 1)
            tell(stage)

    for turn, (early, late) in enumerate(((RIGHT, LEFT), (LEFT, RIGHT))):
        @pl.when(lax.rem(e, 2) == turn)
        def _(early=early, late=late):
            with jax.named_scope("diag"):
                @pl.when(exists[late])
                def _():
                    pl.semaphore_wait(greeted, 1)
                    for band in bands:
                        start(band, lambda band=band: diagonal(band, late))
            with jax.named_scope("hearx"):
                pl.when(2 * e >= easts)(greet)
            with jax.named_scope("early"):
                share(early)
                pl.when(jnp.logical_not(exists[late]))(lambda: share(late))
                strip(early)
                both(far_last)
            with jax.named_scope("hear0"):
                pl.when(2 * e < easts)(greet)
            with jax.named_scope("hear1"):
                for stage in range(max(1, len(stages) - 1), len(stages)):
                    hear(stage - 1)
                    tell(stage)
            with jax.named_scope("late"):
                strip(late)
    total = end[4]
    for row in range(5, J - 4):
        total = total + end[row]

    def rim(side):
        edge_row, outer, two, three, four, sign = ((0, -1, 0, 0, 0, -1.0), (J - 1, J, J - 2, J - 3, J - 4, 1.0))[side]
        pl.when(exists[side] & jnp.logical_not(later))(lambda: count(far_sem.at[BACK[side]], 3 * I + 14))

        @pl.when(exists[side] & later)
        def _():
            count(far_sem.at[BACK[side]], 3 * I + 18)
        beyond = outer + outer - edge_row
        for turn, col in enumerate((-2, I - 1)):
            @pl.when((lax.rem(e, 2) == turn) & exists[side] & later)
            def _(col=col):
                part[side, pl.ds(TILE + col, 3), :] = lone(
                    BACK[side], *(line(level0, r, c, 3) for r, c in
                                  ((outer, col), (beyond, col), (outer, col - 1), (outer, col + 1))),
                    line(flows.at[0], outer, col, 3), line(flows.at[1], beyond, col, 3))
        update(1, edge_row, 1, -3, I + 6)
        trim(1, edge_row, 1, 3)
        level1[outer + PAD, pl.ds(TILE - 2, I + 4), :] = part[side, pl.ds(TILE - 2, I + 4), :] + (
            RATE + sign * line(flows.at[0], outer, -2, I + 4)) * line(level0, edge_row, -2, I + 4)
        trim(1, outer, 1, 2)
        pl.when(jnp.logical_not(exists[side]))(lambda: clear(level1, outer, 1, -2, I + 4))
        update(2, two, 2, -2, I + 4)
        trim(2, two, 2, 2)
        start(side, lambda: [second(side)])
        update(3, three, 3, -1, I + 2)
        trim(3, three, 3, 1)
        level3[outer + PAD, pl.ds(TILE - 1, I + 2), :] = zeros((I + 2, M))

        @pl.when(exists[side])
        def _():
            level3[outer + PAD, pl.ds(TILE - 1, I + 2), :] = (
                RATE + sign * line(flows.at[0], outer, -1, I + 2)) * line(level2, edge_row, -1, I + 2)

        trim(3, outer, 1, 1)
        update(4, four, 4, 0, I)

    for turn, sides in enumerate(((LOWER, UPPER), (UPPER, LOWER))):
        @pl.when(lax.rem(s, 2) == turn)
        def _(sides=sides):
            for number, side in enumerate(sides):
                with jax.named_scope(f"rim{number}"):
                    rim(side)
    for row in (*range(4), *range(J - 4, J)):
        total = total + end[row]
    with jax.named_scope("spill"):
        for side, outer, last, sign in ((LOWER, -1, -2, -1.0), (UPPER, J, J + 1, 1.0)):
            @pl.when(exists[side])
            def _(side=side, outer=outer, last=last, sign=sign):
                count(last_sem.at[BACK[side]], 2 * I)
                value = advance(level3, flows, outer, 1, 0, I)[0]
                spill[side] = value + (RATE + sign * line(flows.at[0], last, 0, I)) * line(level3, outer, 0, I)

        own[...] = total + spill[LOWER] + spill[UPPER]

    def total_copy(source, other):
        return pltpu.make_async_remote_copy(
            src_ref=own, dst_ref=totals.at[source], send_sem=load_sem.at[2], recv_sem=total_recv,
            device_id={"south": other, "east": e}, device_id_type=MESH)

    with jax.named_scope("give"):
        reach = stages[-1] if stages else souths
        odd, even = (souths - s) // 2, (souths - s - 1) // 2
        near_odd, near_even = jnp.minimum(odd, (reach + 1) // 2), jnp.minimum(even, reach // 2)

        def give(lower, upper, distance):
            def one(turn, _):
                total_copy(s, s + distance(turn)).start()
                return 0

            lax.fori_loop(lower, upper, one, 0)

        give(0, near_odd, lambda turn: 2 * turn + 1)
        give(0, near_even, lambda turn: 2 * (near_even - turn))
        if stages:
            hear(len(stages) - 1)
            give(near_odd, odd, lambda turn: 2 * turn + 1)
            give(0, even - near_even, lambda turn: 2 * (even - turn))

    with jax.named_scope("recv2"):
        for side in (LOWER, UPPER):
            pl.when(exists[side])(lambda side=side: second(BACK[side]).wait_recv())
    with jax.named_scope("reply"):
        for side, sign, edge, inner, outer, close, away in (
            (LOWER, 1.0, 0, 1, -1, 1, 0), (UPPER, -1.0, J - 1, J - 2, J, 0, 1),
        ):
            @pl.when(exists[side])
            def _(side=side, sign=sign, edge=edge, inner=inner, outer=outer, close=close, away=away):
                def near_at(di, cols=I, col=0):
                    return halo[side, close, pl.ds(TILE + col + di, cols), :]

                def pair(value, at_outer):
                    none = jnp.zeros_like(value)
                    lower = (side == LOWER)
                    return (value, none) if lower else (none, value)

                reply[side, pl.ds(TILE - 1, I + 2), :] = (
                    RATE + sign * line(flows.at[0], edge, -1, I + 2)) * near_at(0, I + 2, -1)
                far = halo[side, away, pl.ds(TILE, I), :]
                outside = step(near_at(0), *pair(far, True), near_at(-1), near_at(1),
                               line(flows.at[0], outer, 0, I), line(flows.at[1], outer, 0, I))

                def here(di):
                    return reply[side, pl.ds(TILE + di, I), :]

                first = step(here(0), *pair(outside, False), here(-1), here(1),
                             line(flows.at[0], edge, 0, I), line(flows.at[1], edge, 0, I))
                then = (RATE + sign * line(flows.at[0], inner, 0, I)) * here(0)
                end[edge] = end[edge] + first
                end[inner] = end[inner] + then
                if side == LOWER:
                    spill[LOWER] = spill[LOWER] - first - then

    with jax.named_scope("sent"):
        one, two = exists[LOWER], exists[UPPER]
        for has, cells, slanted in ((later, 7 * I + 12, 10), (jnp.logical_not(later), 7 * I + 18, 0)):
            for many, number in ((one != two, 1), (one & two, 2)):
                @pl.when(has & many)
                def _(cells=cells, slanted=slanted, number=number):
                    count(load_sem.at[0], number * cells)
                    if slanted:
                        count(load_sem.at[3], number * slanted)
        sooner = ((lax.rem(e, 2) == 0) & exists[RIGHT]) | ((lax.rem(e, 2) == 1) & exists[LEFT])
        pl.when(sooner & later)(lambda: count(load_sem.at[1], 20 * (J + 1)))
        pl.when(sooner & jnp.logical_not(later))(lambda: count(load_sem.at[1], 10 * (J + 2)))
        pl.when(later & jnp.logical_not(sooner))(lambda: count(load_sem.at[1], 10 * J))
    with jax.named_scope("take"):
        for given in range(1, souths):
            piece = totals.at[pl.ds(0, given)]
            pl.when(s == given)(lambda piece=piece: pltpu.make_async_copy(piece, piece, total_recv).wait())
        before[...] = lax.fori_loop(0, s, lambda source, state: state + totals[source], spill[LOWER])
    for given in range(1, souths):
        piece = totals.at[pl.ds(0, given)]
        pl.when(s == souths - 1 - given)(lambda piece=piece: pltpu.make_async_copy(piece, piece, load_sem.at[2]).wait())


def write_out(scale, before, end, running_out, end_out, running, sems):
    J = end.shape[0]
    parts = 1
    rows = J // parts
    copies = [pltpu.make_async_copy(end, end_out, sems.at[0])]
    copies[0].start()
    state = before[...]
    for part in range(parts):
        for row in range(part * rows, (part + 1) * rows):
            state = state + end[row]
            running[row] = state * scale
        area = pl.ds(part * rows, rows)
        copies.append(pltpu.make_async_copy(running.at[area], running_out.at[area], sems.at[1 + part]))
        copies[-1].start()
    for copy in copies:
        copy.wait()


def per_device(souths, easts, tracer, flow_j, flow_i):
    J, I, M = tracer.shape
    out = jax.ShapeDtypeStruct((J, I, M), jnp.float32)
    padded = (J + 2 * PAD, I + 2 * TILE, M)
    dma = pltpu.SemaphoreType.DMA
    results = pl.pallas_call(
        functools.partial(kernel, souths, easts),
        out_shape=(jax.ShapeDtypeStruct((I, M), jnp.float32), out),
        in_specs=[pl.BlockSpec(memory_space=pl.ANY)] * 3,
        out_specs=(pl.BlockSpec(memory_space=pltpu.VMEM),) * 2,
        scratch_shapes=[pltpu.VMEM(padded, jnp.float32)] * 4
        + [
            pltpu.VMEM((2,) + padded, jnp.float32),
            pltpu.VMEM((2, 2) + padded[1:], jnp.float32),
            pltpu.VMEM((2,) + padded[1:], jnp.float32),
            pltpu.VMEM((2, I, M), jnp.float32),
            pltpu.VMEM((2,) + padded[1:], jnp.float32),
            pltpu.VMEM((2, 2, 2, TILE, M), jnp.float32),
            pltpu.VMEM((2, 2, 2, TILE, M), jnp.float32),
            pltpu.VMEM((2,) + padded[1:], jnp.float32),
            pltpu.VMEM((2, 2, TILE, M), jnp.float32),
            pltpu.VMEM((max(20 * (J + 2), 14 * I + 40), M), jnp.float32),
            pltpu.VMEM((I, M), jnp.float32),
            pltpu.VMEM((souths, I, M), jnp.float32),
            pltpu.SemaphoreType.REGULAR((max(1, (souths - 1).bit_length()),)),
            dma((4,)), dma, dma((2,)), dma((2,)), dma((2,)), dma((2,)), dma, pltpu.SemaphoreType.REGULAR,
        ],
        compiler_params=pltpu.CompilerParams(collective_id=0, has_side_effects=True,
                                             vmem_limit_bytes=106 * 2 ** 19),
    )(tracer, flow_j, flow_i)
    return pl.pallas_call(
        functools.partial(write_out, 1.0 / (J * souths)),
        out_shape=(out, out),
        in_specs=[pl.BlockSpec(memory_space=pltpu.VMEM)] * 2,
        out_specs=(pl.BlockSpec(memory_space=pl.ANY),) * 2,
        scratch_shapes=[pltpu.VMEM((J, I, M), jnp.float32), pltpu.SemaphoreType.DMA((2,))],
        compiler_params=pltpu.CompilerParams(vmem_limit_bytes=2 ** 21),
    )(*results)


def solution(mesh):
    spec = P("south", "east", None)
    body = functools.partial(per_device, mesh.shape["south"], mesh.shape["east"])
    return jax.shard_map(body, mesh=mesh, in_specs=(spec,) * 3, out_specs=(spec,) * 2, check_vma=False)
```
